512 devices in a mesh: blk: 64 (over z, y_hi, core), rep: 8 (over y_lo, x).
Axes of the slice: x: 4, y: 8 (y_hi: 4, y_lo: 2; y = y_hi * 2 + y_lo), z: 8, core: 2. Of those that a mesh axis runs over, the one named last changes fastest.
Arguments:
- raw_integrals: float32 [64, 1024, 512], P(None, 'blk'), may hold values from -0.6 to 0.6
- virtual_coeffs: float32 [512, 256], P(None, 'rep'), may hold values from -0.25 to 0.25
- metric_root: float32 [1024, 1024], P(None, 'rep'), may hold values from -1 to 3, as said below
- occ_energies: float32 [64], P('blk'), may hold values from -2 to -0.5
- virt_energies: float32 [256], replicated, may hold values from 0.2 to 3
Outputs:
- gamma: float32 [64, 256, 1024], P('blk', None, 'rep')
The draws below stay inside these ranges and needn't reach their ends.
Inputs may be any that keep to these rules, and one draw needn't show every extreme that they name: metric_root is exactly symmetric.
All inputs are finite; a program needn't handle non-finite values.
Results may differ from the reference program's by a relative error of at most 0.0001.
Values sent between devices are 32-bit elements; how exact they have to be, the bound alone decides.
A program may use at most 64 MiB of HBM per device.

```python
import math
import jax
import jax.numpy as jnp
from jax import lax

OCC_DEV = 1
V = 256
NAUX = 1024
NAO = 512
OCC = 64
PAIR_BLOCKS = 16


def draw_metric_root(key, part):
    first_key = jax.random.fold_in(key, 11)
    second_key = jax.random.fold_in(key, 23)
    normal_part = jnp.clip(jax.random.normal(first_key, (NAUX, NAUX), jnp.float32), -4.0, 4.0)
    diagonal = jax.random.uniform(second_key, (NAUX,), jnp.float32, 1.0, 2.0)
    symmetric = 0.3 * (normal_part + normal_part.T) / math.sqrt(NAUX)
    return symmetric + jnp.diag(diagonal)


def block_levels(own_key, extent, shards, low, largest):
    def one(axis_at, blocks):
        heights = jax.random.uniform(jax.random.fold_in(jax.random.fold_in(own_key, 6), axis_at), (blocks,), jnp.float32, low / len(shards), largest / len(shards))
        return jnp.repeat(jnp.exp(heights), extent[axis_at] // blocks).reshape((-1,) + (1,) * (len(extent) - axis_at - 1))

    level = one(*shards[0])
    for cut in shards[1:]:
        level = level * one(*cut)
    return level


def noise(rng, dims, scale, most, cuts=(), dtype=jnp.bfloat16):
    entries = scale * jax.random.normal(rng, dims, jnp.float32)
    if cuts:
        entries = entries * block_levels(rng, dims, cuts, -0.22, 0.18)
    return jnp.clip(entries, -most, most).astype(dtype)


def setup_inputs(seed: int = 0) -> dict:
    arg_keys = jax.random.split(jax.random.key(seed), 6)
    raw_integrals = noise(arg_keys[0], (OCC, NAUX, NAO), 0.1, 0.6, ((1, 64),), jnp.float32)
    virtual_coeffs = noise(arg_keys[1], (NAO, V), NAO ** -0.5, 0.25, ((1, 8),), jnp.float32)
    metric_root = draw_metric_root(jax.random.fold_in(arg_keys[5], 71), 0)
    occ_energies = jnp.clip(-2.0 + 1.5 * jax.random.uniform(arg_keys[3], (OCC,), jnp.float32) ** block_levels(arg_keys[3], (OCC,), ((0, 64),), -0.2, 0.2), -2.0, -0.5)
    virt_energies = jnp.clip(jax.random.uniform(arg_keys[4], (V,), jnp.float32, 0.2, 3.0), 0.2, 3.0)
    return {"raw_integrals": raw_integrals, "virtual_coeffs": virtual_coeffs, "metric_root": metric_root, "occ_energies": occ_energies, "virt_energies": virt_energies}


def reference(raw_integrals, virtual_coeffs, metric_root, occ_energies, virt_energies):
    highest = lax.Precision.HIGHEST
    halfway = jnp.einsum("ipm,ma->ipa", raw_integrals, virtual_coeffs, precision=highest)
    fitted = jnp.einsum("ipa,pq->iaq", halfway, metric_root, precision=highest)
    spread = virt_energies[:, None] + virt_energies[None, :]
    block_count = OCC // OCC_DEV
    blocks = fitted.reshape(block_count, OCC_DEV, V, NAUX)
    eps_blocks = occ_energies.reshape(block_count, OCC_DEV)
    gradient = jnp.zeros(blocks.shape, jnp.float32)
    for distance in range(PAIR_BLOCKS):
        other = jnp.roll(blocks, distance, axis=0)
        other_eps = jnp.roll(eps_blocks, distance, axis=0)
        coulomb = jnp.einsum("kxaq,kybq->kxyab", blocks, other, precision=highest)
        denominator = spread[None, None, None] - eps_blocks[:, :, None, None, None] - other_eps[:, None, :, None, None]
        amplitude = (2.0 * coulomb - jnp.swapaxes(coulomb, 3, 4)) / denominator
        gradient = gradient + jnp.einsum("kxyab,kybq->kxaq", amplitude, other, precision=highest)
    return gradient.reshape(OCC, V, NAUX)
```

```python
import jax
import jax.numpy as jnp
from jax import lax
from jax.experimental import pallas as pl
from jax.experimental.pallas import tpu as pltpu
from jax.sharding import Mesh
from jax.sharding import PartitionSpec as P

F32 = jnp.float32
BF16 = jnp.bfloat16
MESH = pl.DeviceIdType.MESH
Z, YH, CO, YL, X = 8, 4, 2, 2, 4
BLK = ("z", "yh", "co")
REP = ("yl", "x")
NI, NP, NM, NA, NQ = 64, 16, 512, 32, 128
HOLDER = (0, 1, 3, 4, 6, 2, 7, 5)
DISTANCE = (0, 1, 5, 2, 3, 7, 4, 6)


def halves(v):
    high = v.astype(BF16)
    return high, (v - high.astype(F32)).astype(BF16)


def mm(a, b):
    return jnp.dot(a, b, preferred_element_type=F32)


def mm3(a, b):
    return mm(a[0], b[0]) + (mm(a[0], b[1]) + mm(a[1], b[0]))


def mm_nt(a, b):
    return lax.dot_general(a, b, (((1,), (1,)), ((), ())), preferred_element_type=F32)


def strided(ref, count, k):
    parts = []
    for part in range(count):
        rows = [ref[part, pl.ds(4 * p + k, NI, stride=NP), :] for p in range(4)]
        parts.append(jnp.concatenate(rows, axis=0))
    return jnp.concatenate(parts, axis=1)


def pick(index, table):
    out = table[-1]
    for at in range(len(table) - 2, -1, -1):
        out = jnp.where(index == at, table[at], out)
    return jnp.int32(out)


def kernel(
    raw_hbm, c_ref, m_hbm, occ_ref, virt_ref, out_ref,
    raw_v, mbuf, hsend, hx, sbuf, fbuf, jhi, jlo, thi, tlo, esend, ebuf, g, grecv,
    local_sem, a2a_send, a2a_recv, m_send, m_recv, e_send, e_recv, x_send, x_recv,
    s_send, s_recv, f_send, f_recv, p_send, d_send, d_recv, g_send, g_recv,
):
    z, yh, co = lax.axis_index("z"), lax.axis_index("yh"), lax.axis_index("co")
    yl, x = lax.axis_index("yl"), lax.axis_index("x")
    me = (z * YH + yh) * CO + co
    chip = z * YH + yh
    rep = yl * X + x
    is_root = rep == HOLDER[0]

    def remote(src, dst, ss, rs, **where):
        return pltpu.make_async_remote_copy(
            src_ref=src, dst_ref=dst, send_sem=ss, recv_sem=rs, device_id=where, device_id_type=MESH
        )

    raw_copies = []
    for part in range(4):
        raw_copies.append(
            pltpu.make_async_copy(raw_hbm.at[:, pl.ds(128 * part, 128)], raw_v.at[part], local_sem.at[1 + part])
        )
        raw_copies[-1].start()
    m_copy = pltpu.make_async_copy(m_hbm, mbuf.at[yl], local_sem.at[0])
    m_copy.start()

    barrier = pltpu.get_barrier_semaphore()

    def greet_blk(t, _):
        other = lax.rem(me + t, NI)
        pl.semaphore_signal(
            barrier, inc=1, device_id={"z": other // 8, "yh": lax.rem(other // 2, YH), "co": lax.rem(other, 2)},
            device_id_type=MESH,
        )
        return 0

    lax.fori_loop(1, NI, greet_blk, 0)

    def greet_plane(t, _):
        other = lax.rem(rep + t % 8, 8)
        pl.semaphore_signal(
            barrier, inc=1,
            device_id={"yh": lax.rem(yh + t // 8, YH), "yl": other // X, "x": lax.rem(other, X)},
            device_id_type=MESH,
        )
        return 0

    for block in range(YH):
        lax.fori_loop(8 * block + 1, 8 * block + 8, greet_plane, 0)

    esend[...] = jnp.full((8, 128), occ_ref[0, 0], F32)

    c_high, c_low = halves(c_ref[...])
    for copy in raw_copies:
        copy.wait()
    total = jnp.zeros((4 * NI, 128), F32)
    for k in range(4):
        place = (
            lax.broadcasted_iota(jnp.int32, (NA, 128), 1) == lax.broadcasted_iota(jnp.int32, (NA, 128), 0) + NA * k
        ).astype(F32).astype(BF16)
        right = (mm(c_high, place).astype(BF16), mm(c_low, place).astype(BF16))
        rows = strided(raw_v, 4, k)
        total = total + mm3(halves(rows), right)
    for p in range(4):
        hsend[:, p, :] = total[NI * p : NI * (p + 1)]

    pl.semaphore_wait(barrier, NI - 1 + 28)

    def send_half(t, _):
        other = lax.rem(me + t, NI)
        remote(
            hsend.at[other], hx.at[x, me], a2a_send, a2a_recv,
            z=other // 8, yh=lax.rem(other // 2, YH), co=lax.rem(other, 2),
        ).start()
        return 0

    lax.fori_loop(1, NI, send_half, 0)
    hx[x, me] = hsend[me]

    y = yh * YL + yl
    metric = []
    for side, to in ((0, lax.rem(y + 1, 8)), (1, lax.rem(y + 7, 8))):
        rows_of = pl.ds(side * 512, 512)
        copy = remote(
            m_hbm.at[rows_of], mbuf.at[yl, rows_of], m_send.at[side], m_recv.at[side],
            yh=to // YL, yl=lax.rem(to, YL),
        )
        copy.start()
        metric.append(copy)

    distance = pick(rep, DISTANCE)
    ahead = chip + distance
    energies = []
    for core in range(CO):
        energies.append((
            jnp.logical_not(is_root),
            remote(
                esend, ebuf.at[co], e_send.at[core], e_recv.at[co],
                z=lax.rem(ahead // YH, Z), yh=lax.rem(ahead, YH), co=jnp.int32(core),
            ),
        ))
    energies.append((
        jnp.logical_and(is_root, co == 1),
        remote(esend, ebuf.at[1], e_send.at[0], e_recv.at[1], z=lax.rem(z + 2, Z), co=jnp.int32(0)),
    ))
    energies.append((
        jnp.logical_and(is_root, co == 0),
        remote(esend, ebuf.at[0], e_send.at[0], e_recv.at[0], co=jnp.int32(1)),
    ))
    for when, copy in energies:
        @pl.when(when)
        def _(copy=copy):
            copy.start()

    @pl.when(is_root)
    def _():
        ebuf[co] = esend[...]

    remote(
        hx.at[x, pl.ds(0, NI - 1)], hx.at[x, pl.ds(0, NI - 1)], a2a_send, a2a_recv, co=1 - co
    ).wait_recv()
    gathers = []
    for step in (2, 1, 3):
        copy = remote(hx.at[x], hx.at[x], x_send.at[step], x_recv.at[x], x=lax.rem(x + step, X))
        copy.start()
        gathers.append(copy)
    m_copy.wait()
    for copy in metric:
        copy.wait_recv()
    for step in (1, 3, 2):
        origin = lax.rem(x + step, X)
        remote(hx.at[origin], hx.at[origin], x_send.at[step], x_recv.at[origin], x=origin).wait_recv()

    turned = []
    for xx in range(X):
        block = jnp.concatenate([hx[xx, :, p, :] for p in range(4)], axis=0)
        turned.append(block.T)
    part = jnp.zeros((128, 256), F32)
    for k in range(4):
        left = jnp.concatenate([t[NA * k : NA * (k + 1), :] for t in turned], axis=0)
        right = strided(mbuf, 2, k)
        part = part + mm3(halves(left), halves(right))
    my_rows = pl.ds(pl.multiple_of(yl * 128, 128), 128)
    sbuf[0] = part
    fbuf[0, x, my_rows, :] = part

    up = lax.rem(z + 1, Z)
    sends = []

    def launch(copy, when=None):
        sends.append((copy, when))
        if when is None:
            copy.start()
        else:
            @pl.when(when)
            def _():
                copy.start()

    def to_holder(slot, index, steps, holder, when=None):
        launch(
            remote(
                sbuf.at[slot], fbuf.at[1 + co, x, my_rows], p_send.at[index], f_recv.at[1, rep],
                yh=lax.rem(yh + steps, YH), yl=holder // X, x=lax.rem(holder, X),
            ),
            when,
        )

    launch(remote(sbuf.at[0], sbuf.at[1], s_send.at[0], s_recv.at[0], z=up))
    for step in range(1, 4):
        to_holder(0, step - 1, step, jnp.int32(HOLDER[step]), yh + step < YH)
    for step in (6, 2, 5, 7, 3, 1, 4):
        other = lax.rem(rep + step, 8)
        launch(
            remote(
                fbuf.at[0, x, my_rows], fbuf.at[0, x, my_rows], f_send.at[step], f_recv.at[0, rep],
                yl=other // X, x=lax.rem(other, X),
            )
        )

    remote(sbuf.at[1], sbuf.at[1], s_send.at[0], s_recv.at[0], z=up).wait_recv()
    launch(remote(sbuf.at[1], sbuf.at[2], s_send.at[1], s_recv.at[1], z=up))
    for step in (2, 1, 3):
        holder = jnp.where(yh + step >= YH, HOLDER[step], HOLDER[step + 4])
        to_holder(1, 3 + step, step, holder)
    to_holder(1, 3, 0, jnp.int32(HOLDER[4]), rep != HOLDER[4])

    @pl.when(rep == HOLDER[4])
    def _():
        fbuf[1 + co, x, my_rows, :] = sbuf[1]

    remote(sbuf.at[2], sbuf.at[2], s_send.at[1], s_recv.at[1], z=up).wait_recv()
    for step in (2, 1, 3):
        to_holder(2, 7 + step, step, jnp.int32(HOLDER[step + 4]), yh + step >= YH)
    to_holder(2, 7, 0, jnp.int32(HOLDER[0]), jnp.logical_and(co == 1, jnp.logical_not(is_root)))

    @pl.when(jnp.logical_and(is_root, co == 1))
    def _():
        fbuf[2, x, my_rows, :] = sbuf[2]

    own_first = jnp.logical_and(is_root, co == 0)
    kind = jnp.where(own_first, 0, 1)
    source = jnp.where(own_first, 0, 1 + co)
    here = jnp.logical_or(is_root, rep == HOLDER[4])

    def block_of(slot, origin):
        return fbuf.at[slot, lax.rem(origin, X), pl.ds(pl.multiple_of(origin // X * 128, 128), 128)]

    def pass_on(t, _):
        origin = lax.rem(rep + t, 8)

        @pl.when(jnp.logical_not(jnp.logical_and(origin == rep, here)))
        def _():
            remote(
                block_of(source, origin), block_of(source, origin), f_send.at[0], f_recv.at[kind, origin],
                co=1 - co,
            ).wait_recv()

        remote(
            block_of(source, origin), block_of(1 + co, origin), d_send.at[origin], d_recv.at[origin], co=1 - co
        ).start()
        return 0

    lax.fori_loop(0, 8, pass_on, 0)

    def own_arrived(t, _):
        origin = lax.rem(rep + t, 8)
        remote(
            block_of(0, origin), block_of(0, origin), f_send.at[0], f_recv.at[0, origin], co=1 - co
        ).wait_recv()
        return 0

    @pl.when(jnp.logical_not(own_first))
    def _():
        lax.fori_loop(1, 8, own_arrived, 0)

    for core in range(CO):
        expected = jnp.logical_or(jnp.logical_not(is_root), co != core)

        @pl.when(expected)
        def _(core=core):
            remote(esend, ebuf.at[core], e_send.at[0], e_recv.at[core], co=1 - co).wait_recv()

    row = jnp.broadcast_to(virt_ref[...], (256, 256))
    spread = row + row.T - occ_ref[0, 0]

    def pair(order):
        which = co if order == 0 else 1 - co
        slot = jnp.where(jnp.logical_and(is_root, co == which), 0, 1 + which)
        coulomb = jnp.zeros((256, 256), F32)
        for xx in range(X):
            ih, il = halves(fbuf[0, xx])
            jh, jl = halves(fbuf[slot, xx])
            jhi[order, xx] = jh
            jlo[order, xx] = jl
            coulomb = coulomb + (mm_nt(ih, jh) + (mm_nt(ih, jl) + mm_nt(il, jh)))
        amplitude = (2.0 * coulomb - coulomb.T) / (spread - ebuf[which][0:1, 0:1])
        th, tl = halves(amplitude)
        thi[order] = th
        tlo[order] = tl

    pair(0)

    def twin_arrived(t, _):
        remote(
            block_of(2 - co, t), block_of(2 - co, t), d_send.at[t], d_recv.at[t], co=1 - co
        ).wait_recv()
        return 0

    lax.fori_loop(0, 8, twin_arrived, 0)
    pair(1)

    for step in (2, 1, 3, 0):
        xx = lax.rem(x + step, X)
        block = jnp.zeros((256, 256), F32)
        for order in range(2):
            block = block + mm3((thi[order], tlo[order]), (jhi[order, xx], jlo[order, xx]))
        for half in range(YL):
            g[xx, half] = block[:, half * NQ : (half + 1) * NQ]
        if step:
            for half in range(YL):
                launch(
                    remote(
                        g.at[xx, half], grecv.at[rep], g_send.at[YL * step + half], g_recv.at[rep],
                        yl=jnp.int32(half), x=xx,
                    )
                )
        else:
            launch(
                remote(g.at[xx, 1 - yl], grecv.at[rep], g_send.at[0], g_recv.at[rep], yl=1 - yl, x=xx)
            )
            grecv[rep] = g[xx, yl]

    def gradient_arrived(t, _):
        origin = lax.rem(rep + t, 8)
        remote(grecv.at[origin], grecv.at[origin], g_send.at[0], g_recv.at[origin], co=1 - co).wait_recv()
        return 0

    lax.fori_loop(1, 8, gradient_arrived, 0)
    result = grecv[0]
    for origin in range(1, 8):
        result = result + grecv[origin]
    out_ref[...] = result

    remote(
        hsend.at[pl.ds(0, NI - 1)], hx.at[x, pl.ds(0, NI - 1)], a2a_send, a2a_recv, co=1 - co
    ).wait_send()
    for copy in metric + gathers:
        copy.wait_send()
    for when, copy in energies:
        @pl.when(when)
        def _(copy=copy):
            copy.wait_send()
    for copy, when in sends:
        if when is None:
            copy.wait_send()
        else:
            @pl.when(when)
            def _(copy=copy):
                copy.wait_send()

    def passed(t, _):
        remote(
            block_of(source, t), block_of(1 + co, t), d_send.at[t], d_recv.at[t], co=1 - co
        ).wait_send()
        return 0

    lax.fori_loop(0, 8, passed, 0)


def per_device(raw_integrals, virtual_coeffs, metric_root, occ_energies, virt_energies):
    vmem = pl.BlockSpec(memory_space=pltpu.VMEM)
    anywhere = pl.BlockSpec(memory_space=pl.ANY)
    dma = pltpu.SemaphoreType.DMA
    out = pl.pallas_call(
        kernel,
        out_shape=jax.ShapeDtypeStruct((256, NQ), F32),
        in_specs=[anywhere, vmem, anywhere, pl.BlockSpec(memory_space=pltpu.SMEM), vmem],
        out_specs=vmem,
        scratch_shapes=[
            pltpu.VMEM((4, NI * NP, 128), F32),
            pltpu.VMEM((YL, 1024, NQ), F32),
            pltpu.VMEM((NI, 4, 128), F32),
            pltpu.VMEM((X, NI, 4, 128), F32),
            pltpu.VMEM((3, 128, 256), F32),
            pltpu.VMEM((3, X, 256, 256), F32),
            pltpu.VMEM((2, X, 256, 256), BF16),
            pltpu.VMEM((2, X, 256, 256), BF16),
            pltpu.VMEM((2, 256, 256), BF16),
            pltpu.VMEM((2, 256, 256), BF16),
            pltpu.VMEM((8, 128), F32),
            pltpu.VMEM((2, 8, 128), F32),
            pltpu.VMEM((X, YL, 256, NQ), F32),
            pltpu.VMEM((8, 256, NQ), F32),
            dma((5,)), dma, dma, dma((2,)), dma((2,)), dma((2,)), dma((2,)), dma((4,)), dma((4,)),
            dma((2,)), dma((2,)), dma((8,)), dma((2, 8)), dma((11,)), dma((8,)), dma((8,)), dma((8,)), dma((8,)),
        ],
        compiler_params=pltpu.CompilerParams(
            collective_id=0, has_side_effects=True, vmem_limit_bytes=48 * 1024 * 1024
        ),
        name="gradient_density",
    )(
        raw_integrals.reshape(NI * NP, NM), virtual_coeffs, metric_root,
        occ_energies.reshape(1, 1), virt_energies.reshape(1, 256),
    )
    return out[None]


def solution(mesh):
    finer = Mesh(mesh.devices.reshape(Z, YH, CO, YL, X), BLK + REP)
    return jax.shard_map(
        per_device,
        mesh=finer,
        in_specs=(P(None, BLK, None), P(None, REP), P(None, REP), P(BLK), P()),
        out_specs=P(BLK, None, REP),
        check_vma=False,
    )
```

```python
import jax
import jax.numpy as jnp
from jax import lax
from jax.experimental import pallas as pl
from jax.experimental.pallas import tpu as pltpu
from jax.sharding import Mesh
from jax.sharding import PartitionSpec as P

F32 = jnp.float32
BF16 = jnp.bfloat16
MESH = pl.DeviceIdType.MESH
Z, YH, CO, YL, X = 8, 4, 2, 2, 4
BLK = ("z", "yh", "co")
REP = ("yl", "x")
NI, NP, NM, NA, NQ = 64, 16, 512, 32, 128
HOLDER = (0, 1, 3, 4, 6, 2, 7, 5)
DISTANCE = (0, 1, 5, 2, 3, 7, 4, 6)


def halves(v):
    high = v.astype(BF16)
    return high, (v - high.astype(F32)).astype(BF16)


def mm(a, b):
    return jnp.dot(a, b, preferred_element_type=F32)


def mm3(a, b):
    return mm(a[0], b[0]) + (mm(a[0], b[1]) + mm(a[1], b[0]))


def mm_nt(a, b):
    return lax.dot_general(a, b, (((1,), (1,)), ((), ())), preferred_element_type=F32)


def strided(ref, count, k):
    parts = []
    for part in range(count):
        rows = [ref[part, pl.ds(4 * p + k, NI, stride=NP), :] for p in range(4)]
        parts.append(jnp.concatenate(rows, axis=0))
    return jnp.concatenate(parts, axis=1)


def pick(index, table):
    out = table[-1]
    for at in range(len(table) - 2, -1, -1):
        out = jnp.where(index == at, table[at], out)
    return jnp.int32(out)


def kernel(
    raw_hbm, c_hbm, m_hbm, occ_ref, virt_hbm, out_ref,
    raw_v, c_v, virt_v, mbuf, hsend, hx, sbuf, fbuf, jhi, jlo, thi, tlo, esend, ebuf, g, grecv,
    local_sem, a2a_send, a2a_recv, m_send, m_recv, e_send, e_recv, x_send, x_recv,
    s_send, s_recv, f_send, f_recv, p_send, d_send, d_recv, g_send, g_recv,
):
    z, yh, co = lax.axis_index("z"), lax.axis_index("yh"), lax.axis_index("co")
    yl, x = lax.axis_index("yl"), lax.axis_index("x")
    me = (z * YH + yh) * CO + co
    chip = z * YH + yh
    rep = yl * X + x
    is_root = rep == HOLDER[0]

    def remote(src, dst, ss, rs, **where):
        return pltpu.make_async_remote_copy(
            src_ref=src, dst_ref=dst, send_sem=ss, recv_sem=rs, device_id=where, device_id_type=MESH
        )

    c_copy = pltpu.make_async_copy(c_hbm, c_v, local_sem.at[5])
    c_copy.start()
    raw_copies = []
    for part in range(4):
        raw_copies.append(
            pltpu.make_async_copy(raw_hbm.at[:, pl.ds(128 * part, 128)], raw_v.at[part], local_sem.at[1 + part])
        )
        raw_copies[-1].start()
    m_copy = pltpu.make_async_copy(m_hbm, mbuf.at[yl], local_sem.at[0])
    m_copy.start()
    virt_copy = pltpu.make_async_copy(virt_hbm, virt_v, local_sem.at[6])
    virt_copy.start()

    zs = [lax.rem(z + step, Z) for step in range(Z)]
    yhs = [lax.rem(yh + step, YH) for step in range(YH)]
    cos = [co, 1 - co]
    yls = [yl, 1 - yl]
    xs = [lax.rem(x + step, X) for step in range(X)]
    across_blk = [(a, b, c) for a in (4, 3, 5, 2, 6, 1, 7, 0) for b in (2, 1, 3, 0) for c in (0, 1)][:-2] + [(0, 0, 1)]
    across_plane = [(a, b, c) for a in (2, 1, 3, 0) for b in (0, 1) for c in (2, 1, 3, 0) if (b, c) != (0, 0)]

    barrier = pltpu.get_barrier_semaphore()
    for a, b, c in across_blk:
        pl.semaphore_signal(
            barrier, inc=1, device_id={"z": zs[a], "yh": yhs[b], "co": cos[c]}, device_id_type=MESH
        )
    for a, b, c in across_plane:
        pl.semaphore_signal(
            barrier, inc=1, device_id={"yh": yhs[a], "yl": yls[b], "x": xs[c]}, device_id_type=MESH
        )

    esend[...] = jnp.full((8, 128), occ_ref[0], F32)

    c_copy.wait()
    c_high, c_low = halves(c_v[...].T)
    for copy in raw_copies:
        copy.wait()
    total = jnp.zeros((4 * NI, 128), F32)
    for k in range(4):
        place = (
            lax.broadcasted_iota(jnp.int32, (NA, 128), 1) == lax.broadcasted_iota(jnp.int32, (NA, 128), 0) + NA * k
        ).astype(F32).astype(BF16)
        right = (mm(c_high, place).astype(BF16), mm(c_low, place).astype(BF16))
        rows = strided(raw_v, 4, k)
        total = total + mm3(halves(rows), right)
    for p in range(4):
        hsend[:, p, :] = total[NI * p : NI * (p + 1)]

    pl.semaphore_wait(barrier, len(across_blk) + len(across_plane))

    for a, b, c in across_blk:
        other = (zs[a] * YH + yhs[b]) * CO + cos[c]
        remote(hsend.at[other], hx.at[x, me], a2a_send, a2a_recv, z=zs[a], yh=yhs[b], co=cos[c]).start()
    hx[x, me] = hsend[me]

    y = yh * YL + yl
    metric = []
    for side, to in ((0, lax.rem(y + 1, 8)), (1, lax.rem(y + 7, 8))):
        rows_of = pl.ds(side * 512, 512)
        copy = remote(
            m_hbm.at[rows_of], mbuf.at[yl, rows_of], m_send.at[side], m_recv.at[side],
            yh=to // YL, yl=lax.rem(to, YL),
        )
        copy.start()
        metric.append(copy)

    distance = pick(rep, DISTANCE)
    ahead = chip + distance
    energies = []
    for core in range(CO):
        energies.append((
            jnp.logical_not(is_root),
            remote(
                esend, ebuf.at[co], e_send.at[core], e_recv.at[co],
                z=lax.rem(ahead // YH, Z), yh=lax.rem(ahead, YH), co=jnp.int32(core),
            ),
        ))
    energies.append((
        jnp.logical_and(is_root, co == 1),
        remote(esend, ebuf.at[1], e_send.at[0], e_recv.at[1], z=lax.rem(z + 2, Z), co=jnp.int32(0)),
    ))
    energies.append((
        jnp.logical_and(is_root, co == 0),
        remote(esend, ebuf.at[0], e_send.at[0], e_recv.at[0], co=jnp.int32(1)),
    ))
    for when, copy in energies:
        @pl.when(when)
        def _(copy=copy):
            copy.start()

    @pl.when(is_root)
    def _():
        ebuf[co] = esend[...]

    remote(
        hx.at[x, pl.ds(0, NI - 1)], hx.at[x, pl.ds(0, NI - 1)], a2a_send, a2a_recv, co=1 - co
    ).wait_recv()
    gathers = []
    for step in (2, 1, 3):
        copy = remote(hx.at[x], hx.at[x], x_send.at[step], x_recv.at[x], x=lax.rem(x + step, X))
        copy.start()
        gathers.append(copy)
    m_copy.wait()
    for copy in metric:
        copy.wait_recv()
    for step in (1, 3, 2):
        origin = lax.rem(x + step, X)
        remote(hx.at[origin], hx.at[origin], x_send.at[step], x_recv.at[origin], x=origin).wait_recv()

    turned = []
    for xx in range(X):
        block = jnp.concatenate([hx[xx, :, p, :] for p in range(4)], axis=0)
        turned.append(block.T)
    part = jnp.zeros((128, 256), F32)
    for k in range(4):
        left = jnp.concatenate([t[NA * k : NA * (k + 1), :] for t in turned], axis=0)
        right = strided(mbuf, 2, k)
        part = part + mm3(halves(left), halves(right))
    my_rows = pl.ds(pl.multiple_of(yl * 128, 128), 128)
    sbuf[0] = part
    fbuf[0, x, my_rows, :] = part

    up = lax.rem(z + 1, Z)
    sends = []

    def launch(copy, when=None):
        sends.append((copy, when))
        if when is None:
            copy.start()
        else:
            @pl.when(when)
            def _():
                copy.start()

    def to_holder(slot, index, steps, holder, when=None):
        launch(
            remote(
                sbuf.at[slot], fbuf.at[1 + co, x, my_rows], p_send.at[index], f_recv.at[1, rep],
                yh=lax.rem(yh + steps, YH), yl=holder // X, x=lax.rem(holder, X),
            ),
            when,
        )

    launch(remote(sbuf.at[0], sbuf.at[1], s_send.at[0], s_recv.at[0], z=up))
    for step in range(1, 4):
        to_holder(0, step - 1, step, jnp.int32(HOLDER[step]), yh + step < YH)
    other_rows = pl.ds(pl.multiple_of((1 - yl) * 128, 128), 128)
    twin = (1 - yl) * X + x
    launch(
        remote(
            fbuf.at[0, x, my_rows], fbuf.at[0, x, my_rows], f_send.at[0], f_recv.at[0, rep], yl=1 - yl
        )
    )
    for step in (2, 1, 3):
        launch(
            remote(
                fbuf.at[0, x, my_rows], fbuf.at[0, x, my_rows], f_send.at[step], f_recv.at[0, rep], x=xs[step]
            )
        )
    remote(
        fbuf.at[0, x, other_rows], fbuf.at[0, x, other_rows], f_send.at[0], f_recv.at[0, twin], co=1 - co
    ).wait_recv()
    for step in (2, 1, 3):
        launch(
            remote(
                fbuf.at[0, x, other_rows], fbuf.at[0, x, other_rows], f_send.at[4 + step], f_recv.at[0, twin],
                x=xs[step],
            )
        )

    remote(sbuf.at[1], sbuf.at[1], s_send.at[0], s_recv.at[0], z=up).wait_recv()
    launch(remote(sbuf.at[1], sbuf.at[2], s_send.at[1], s_recv.at[1], z=up))
    for step in (2, 1, 3):
        holder = jnp.where(yh + step >= YH, HOLDER[step], HOLDER[step + 4])
        to_holder(1, 3 + step, step, holder)
    to_holder(1, 3, 0, jnp.int32(HOLDER[4]), rep != HOLDER[4])

    @pl.when(rep == HOLDER[4])
    def _():
        fbuf[1 + co, x, my_rows, :] = sbuf[1]

    remote(sbuf.at[2], sbuf.at[2], s_send.at[1], s_recv.at[1], z=up).wait_recv()
    for step in (2, 1, 3):
        to_holder(2, 7 + step, step, jnp.int32(HOLDER[step + 4]), yh + step >= YH)
    to_holder(2, 7, 0, jnp.int32(HOLDER[0]), jnp.logical_and(co == 1, jnp.logical_not(is_root)))

    @pl.when(jnp.logical_and(is_root, co == 1))
    def _():
        fbuf[2, x, my_rows, :] = sbuf[2]

    own_first = jnp.logical_and(is_root, co == 0)
    kind = jnp.where(own_first, 0, 1)
    source = jnp.where(own_first, 0, 1 + co)
    here = jnp.logical_or(is_root, rep == HOLDER[4])

    def block_of(slot, origin):
        return fbuf.at[slot, lax.rem(origin, X), pl.ds(pl.multiple_of(origin // X * 128, 128), 128)]

    def pass_on(t, _):
        origin = lax.rem(rep + t, 8)

        known = jnp.logical_or(jnp.logical_and(origin == rep, here), jnp.logical_and(origin == twin, own_first))

        @pl.when(jnp.logical_not(known))
        def _():
            remote(
                block_of(source, origin), block_of(source, origin), f_send.at[0], f_recv.at[kind, origin],
                co=1 - co,
            ).wait_recv()

        remote(
            block_of(source, origin), block_of(1 + co, origin), d_send.at[origin], d_recv.at[origin], co=1 - co
        ).start()
        return 0

    lax.fori_loop(0, 8, pass_on, 0)

    def own_arrived(t, _):
        origin = lax.rem(rep + t, 8)

        @pl.when(origin != twin)
        def _():
            remote(
                block_of(0, origin), block_of(0, origin), f_send.at[0], f_recv.at[0, origin], co=1 - co
            ).wait_recv()

        return 0

    @pl.when(jnp.logical_not(own_first))
    def _():
        lax.fori_loop(1, 8, own_arrived, 0)

    for core in range(CO):
        expected = jnp.logical_or(jnp.logical_not(is_root), co != core)

        @pl.when(expected)
        def _(core=core):
            remote(esend, ebuf.at[core], e_send.at[0], e_recv.at[core], co=1 - co).wait_recv()

    virt_copy.wait()
    row = jnp.broadcast_to(virt_v[...], (256, 256))
    spread = row + row.T - occ_ref[0]

    def pair(order):
        which = co if order == 0 else 1 - co
        slot = jnp.where(jnp.logical_and(is_root, co == which), 0, 1 + which)
        coulomb = jnp.zeros((256, 256), F32)
        for xx in range(X):
            ih, il = halves(fbuf[0, xx])
            jh, jl = halves(fbuf[slot, xx])
            jhi[order, xx] = jh
            jlo[order, xx] = jl
            coulomb = coulomb + (mm_nt(ih, jh) + (mm_nt(ih, jl) + mm_nt(il, jh)))
        amplitude = (2.0 * coulomb - coulomb.T) / (spread - ebuf[which][0:1, 0:1])
        th, tl = halves(amplitude)
        thi[order] = th
        tlo[order] = tl

    pair(0)

    def twin_arrived(t, _):
        remote(
            block_of(2 - co, t), block_of(2 - co, t), d_send.at[t], d_recv.at[t], co=1 - co
        ).wait_recv()
        return 0

    lax.fori_loop(0, 8, twin_arrived, 0)
    pair(1)

    for step in (2, 1, 3, 0):
        xx = lax.rem(x + step, X)
        block = jnp.zeros((256, 256), F32)
        for order in range(2):
            block = block + mm3((thi[order], tlo[order]), (jhi[order, xx], jlo[order, xx]))
        for half in range(YL):
            g[xx, half] = block[:, half * NQ : (half + 1) * NQ]
        if step:
            for half in range(YL):
                launch(
                    remote(
                        g.at[xx, half], grecv.at[rep], g_send.at[YL * step + half], g_recv.at[rep],
                        yl=jnp.int32(half), x=xx,
                    )
                )
        else:
            launch(
                remote(g.at[xx, 1 - yl], grecv.at[rep], g_send.at[0], g_recv.at[rep], yl=1 - yl, x=xx)
            )
            grecv[rep] = g[xx, yl]

    def gradient_arrived(t, _):
        origin = lax.rem(rep + t, 8)
        remote(grecv.at[origin], grecv.at[origin], g_send.at[0], g_recv.at[origin], co=1 - co).wait_recv()
        return 0

    lax.fori_loop(1, 8, gradient_arrived, 0)
    result = grecv[0]
    for origin in range(1, 8):
        result = result + grecv[origin]
    out_ref[...] = result

    remote(
        hsend.at[pl.ds(0, NI - 1)], hx.at[x, pl.ds(0, NI - 1)], a2a_send, a2a_recv, co=1 - co
    ).wait_send()
    for copy in metric + gathers:
        copy.wait_send()
    for when, copy in energies:
        @pl.when(when)
        def _(copy=copy):
            copy.wait_send()
    for copy, when in sends:
        if when is None:
            copy.wait_send()
        else:
            @pl.when(when)
            def _(copy=copy):
                copy.wait_send()

    def passed(t, _):
        remote(
            block_of(source, t), block_of(1 + co, t), d_send.at[t], d_recv.at[t], co=1 - co
        ).wait_send()
        return 0

    lax.fori_loop(0, 8, passed, 0)


def per_device(raw_integrals, virtual_coeffs, metric_root, occ_energies, virt_energies):
    vmem = pl.BlockSpec(memory_space=pltpu.VMEM)
    anywhere = pl.BlockSpec(memory_space=pl.ANY)
    dma = pltpu.SemaphoreType.DMA
    out = pl.pallas_call(
        kernel,
        out_shape=jax.ShapeDtypeStruct((256, NQ), F32),
        in_specs=[anywhere, anywhere, anywhere, pl.BlockSpec(memory_space=pltpu.SMEM), anywhere],
        out_specs=vmem,
        scratch_shapes=[
            pltpu.VMEM((4, NI * NP, 128), F32),
            pltpu.VMEM((NA, NM), F32),
            pltpu.VMEM((1, 256), F32),
            pltpu.VMEM((YL, 1024, NQ), F32),
            pltpu.VMEM((NI, 4, 128), F32),
            pltpu.VMEM((X, NI, 4, 128), F32),
            pltpu.VMEM((3, 128, 256), F32),
            pltpu.VMEM((3, X, 256, 256), F32),
            pltpu.VMEM((2, X, 256, 256), BF16),
            pltpu.VMEM((2, X, 256, 256), BF16),
            pltpu.VMEM((2, 256, 256), BF16),
            pltpu.VMEM((2, 256, 256), BF16),
            pltpu.VMEM((8, 128), F32),
            pltpu.VMEM((2, 8, 128), F32),
            pltpu.VMEM((X, YL, 256, NQ), F32),
            pltpu.VMEM((8, 256, NQ), F32),
            dma((7,)), dma, dma, dma((2,)), dma((2,)), dma((2,)), dma((2,)), dma((4,)), dma((4,)),
            dma((2,)), dma((2,)), dma((8,)), dma((2, 8)), dma((11,)), dma((8,)), dma((8,)), dma((8,)), dma((8,)),
        ],
        compiler_params=pltpu.CompilerParams(
            collective_id=0, has_side_effects=True, vmem_limit_bytes=67043328
        ),
        name="gradient_density",
    )(
        raw_integrals.reshape(NI * NP, NM), virtual_coeffs.T, metric_root,
        occ_energies, virt_energies.reshape(1, 256),
    )
    return out[None]


def solution(mesh):
    finer = Mesh(mesh.devices.reshape(Z, YH, CO, YL, X), BLK + REP)
    return jax.shard_map(
        per_device,
        mesh=finer,
        in_specs=(P(None, BLK, None), P(None, REP), P(None, REP), P(BLK), P()),
        out_specs=P(BLK, None, REP),
        check_vma=False,
    )
```

```python
import jax
import jax.numpy as jnp
from jax import lax
from jax.experimental import pallas as pl
from jax.experimental.pallas import tpu as pltpu
from jax.sharding import Mesh
from jax.sharding import PartitionSpec as P

F32 = jnp.float32
BF16 = jnp.bfloat16
MESH = pl.DeviceIdType.MESH
Z, YH, CO, YL, X = 8, 4, 2, 2, 4
BLK = ("z", "yh", "co")
REP = ("yl", "x")
NI, NP, NM, NA, NQ = 64, 16, 512, 32, 128
HOLDER = (1, 2, 0, 6, 4, 3, 5, 7)
DISTANCE = (2, 0, 1, 5, 4, 6, 3, 7)


def halves(v):
    high = v.astype(BF16)
    return high, (v - high.astype(F32)).astype(BF16)


def mm(a, b):
    return jnp.dot(a, b, preferred_element_type=F32)


def mm3(a, b):
    return mm(a[0], b[0]) + (mm(a[0], b[1]) + mm(a[1], b[0]))


def mm_nt(a, b):
    return lax.dot_general(a, b, (((1,), (1,)), ((), ())), preferred_element_type=F32)


def strided(ref, count, k):
    parts = []
    for part in range(count):
        rows = [ref[part, pl.ds(4 * p + k, NI, stride=NP), :] for p in range(4)]
        parts.append(jnp.concatenate(rows, axis=0))
    return jnp.concatenate(parts, axis=1)


def pick(index, table):
    out = table[-1]
    for at in range(len(table) - 2, -1, -1):
        out = jnp.where(index == at, table[at], out)
    return jnp.int32(out)


def kernel(
    raw_hbm, c_hbm, m_hbm, occ_ref, virt_hbm, out_ref,
    raw_v, c_v, virt_v, mbuf, hsend, hx, sbuf, fbuf, jhi, jlo, thi, tlo, esend, ebuf, g, grecv,
    local_sem, a2a_send, a2a_recv, m_send, m_recv, e_send, e_recv, x_send, x_recv,
    s_send, s_recv, f_send, f_recv, p_send, d_send, d_recv, g_send, g_recv,
):
    z, yh, co = lax.axis_index("z"), lax.axis_index("yh"), lax.axis_index("co")
    yl, x = lax.axis_index("yl"), lax.axis_index("x")
    me = (z * YH + yh) * CO + co
    chip = z * YH + yh
    rep = yl * X + x
    is_root = rep == HOLDER[0]

    def remote(src, dst, ss, rs, **where):
        return pltpu.make_async_remote_copy(
            src_ref=src, dst_ref=dst, send_sem=ss, recv_sem=rs, device_id=where, device_id_type=MESH
        )

    c_copy = pltpu.make_async_copy(c_hbm, c_v, local_sem.at[5])
    c_copy.start()
    raw_copies = []
    for part in range(4):
        raw_copies.append(
            pltpu.make_async_copy(raw_hbm.at[:, pl.ds(128 * part, 128)], raw_v.at[part], local_sem.at[1 + part])
        )
        raw_copies[-1].start()
    m_copy = pltpu.make_async_copy(m_hbm, mbuf.at[yl], local_sem.at[0])
    m_copy.start()
    virt_copy = pltpu.make_async_copy(virt_hbm, virt_v, local_sem.at[6])
    virt_copy.start()

    zs = [lax.rem(z + step, Z) for step in range(Z)]
    yhs = [lax.rem(yh + step, YH) for step in range(YH)]
    cos = [co, 1 - co]
    yls = [yl, 1 - yl]
    xs = [lax.rem(x + step, X) for step in range(X)]
    across_blk = [(a, b, c) for a in (4, 3, 5, 2, 6, 1, 7, 0) for b in (2, 1, 3, 0) for c in (0, 1)][:-2] + [(0, 0, 1)]
    across_plane = [(a, b, c) for a in (2, 1, 3, 0) for b in (0, 1) for c in (2, 1, 3, 0) if (b, c) != (0, 0)]

    barrier = pltpu.get_barrier_semaphore()
    for a, b, c in across_blk:
        pl.semaphore_signal(
            barrier, inc=1, device_id={"z": zs[a], "yh": yhs[b], "co": cos[c]}, device_id_type=MESH
        )
    for a, b, c in across_plane:
        pl.semaphore_signal(
            barrier, inc=1, device_id={"yh": yhs[a], "yl": yls[b], "x": xs[c]}, device_id_type=MESH
        )

    esend[...] = jnp.full((8, 128), occ_ref[0], F32)

    c_copy.wait()
    c_high, c_low = halves(c_v[...].T)
    for copy in raw_copies:
        copy.wait()
    total = jnp.zeros((4 * NI, 128), F32)
    for k in range(4):
        place = (
            lax.broadcasted_iota(jnp.int32, (NA, 128), 1) == lax.broadcasted_iota(jnp.int32, (NA, 128), 0) + NA * k
        ).astype(F32).astype(BF16)
        right = (mm(c_high, place).astype(BF16), mm(c_low, place).astype(BF16))
        rows = strided(raw_v, 4, k)
        total = total + mm3(halves(rows), right)
    for p in range(4):
        hsend[:, p, :] = total[NI * p : NI * (p + 1)]

    pl.semaphore_wait(barrier, len(across_blk) + len(across_plane))

    for a, b, c in across_blk:
        other = (zs[a] * YH + yhs[b]) * CO + cos[c]
        remote(hsend.at[other], hx.at[x, me], a2a_send, a2a_recv, z=zs[a], yh=yhs[b], co=cos[c]).start()
    hx[x, me] = hsend[me]

    y = yh * YL + yl
    metric = []
    for side, to in ((0, lax.rem(y + 1, 8)), (1, lax.rem(y + 7, 8))):
        rows_of = pl.ds(side * 512, 512)
        copy = remote(
            m_hbm.at[rows_of], mbuf.at[yl, rows_of], m_send.at[side], m_recv.at[side],
            yh=to // YL, yl=lax.rem(to, YL),
        )
        copy.start()
        metric.append(copy)

    distance = pick(rep, DISTANCE)
    ahead = chip + distance
    energies = []
    for core in range(CO):
        energies.append((
            jnp.logical_not(is_root),
            remote(
                esend, ebuf.at[co], e_send.at[core], e_recv.at[co],
                z=lax.rem(ahead // YH, Z), yh=lax.rem(ahead, YH), co=jnp.int32(core),
            ),
        ))
    energies.append((
        jnp.logical_and(is_root, co == 1),
        remote(esend, ebuf.at[1], e_send.at[0], e_recv.at[1], z=lax.rem(z + 2, Z), co=jnp.int32(0)),
    ))
    energies.append((
        jnp.logical_and(is_root, co == 0),
        remote(esend, ebuf.at[0], e_send.at[0], e_recv.at[0], co=jnp.int32(1)),
    ))
    for when, copy in energies:
        @pl.when(when)
        def _(copy=copy):
            copy.start()

    @pl.when(is_root)
    def _():
        ebuf[co] = esend[...]

    remote(
        hx.at[x, pl.ds(0, NI - 1)], hx.at[x, pl.ds(0, NI - 1)], a2a_send, a2a_recv, co=1 - co
    ).wait_recv()
    gathers = []
    for step in (2, 1, 3):
        copy = remote(hx.at[x], hx.at[x], x_send.at[step], x_recv.at[x], x=lax.rem(x + step, X))
        copy.start()
        gathers.append(copy)
    m_copy.wait()
    for copy in metric:
        copy.wait_recv()
    for step in (1, 3, 2):
        origin = lax.rem(x + step, X)
        remote(hx.at[origin], hx.at[origin], x_send.at[step], x_recv.at[origin], x=origin).wait_recv()

    turned = []
    for xx in range(X):
        block = jnp.concatenate([hx[xx, :, p, :] for p in range(4)], axis=0)
        turned.append(block.T)
    part = jnp.zeros((128, 256), F32)
    for k in range(4):
        left = jnp.concatenate([t[NA * k : NA * (k + 1), :] for t in turned], axis=0)
        right = strided(mbuf, 2, k)
        part = part + mm3(halves(left), halves(right))
    my_rows = pl.ds(pl.multiple_of(yl * 128, 128), 128)
    sbuf[0] = part
    fbuf[0, x, my_rows, :] = part

    up = lax.rem(z + 1, Z)
    sends = []

    def launch(copy, when=None):
        sends.append((copy, when))
        if when is None:
            copy.start()
        else:
            @pl.when(when)
            def _():
                copy.start()

    def to_holder(slot, index, steps, holder, when=None):
        launch(
            remote(
                sbuf.at[slot], fbuf.at[1 + co, x, my_rows], p_send.at[index], f_recv.at[1, rep],
                yh=lax.rem(yh + steps, YH), yl=holder // X, x=lax.rem(holder, X),
            ),
            when,
        )

    launch(remote(sbuf.at[0], sbuf.at[1], s_send.at[0], s_recv.at[0], z=up))
    for step in range(1, 4):
        to_holder(0, step - 1, step, jnp.int32(HOLDER[step]), yh + step < YH)
    other_rows = pl.ds(pl.multiple_of((1 - yl) * 128, 128), 128)
    twin = (1 - yl) * X + x
    launch(
        remote(
            fbuf.at[0, x, my_rows], fbuf.at[0, x, my_rows], f_send.at[0], f_recv.at[0, rep], yl=1 - yl
        )
    )
    for step in (2, 1, 3):
        launch(
            remote(
                fbuf.at[0, x, my_rows], fbuf.at[0, x, my_rows], f_send.at[step], f_recv.at[0, rep], x=xs[step]
            )
        )
    remote(
        fbuf.at[0, x, other_rows], fbuf.at[0, x, other_rows], f_send.at[0], f_recv.at[0, twin], co=1 - co
    ).wait_recv()
    for step in (2, 1, 3):
        launch(
            remote(
                fbuf.at[0, x, other_rows], fbuf.at[0, x, other_rows], f_send.at[4 + step], f_recv.at[0, twin],
                x=xs[step],
            )
        )

    remote(sbuf.at[1], sbuf.at[1], s_send.at[0], s_recv.at[0], z=up).wait_recv()
    launch(remote(sbuf.at[1], sbuf.at[2], s_send.at[1], s_recv.at[1], z=up))
    for step in (2, 1, 3):
        holder = jnp.where(yh + step >= YH, HOLDER[step], HOLDER[step + 4])
        to_holder(1, 3 + step, step, holder)
    to_holder(1, 3, 0, jnp.int32(HOLDER[4]), rep != HOLDER[4])

    @pl.when(rep == HOLDER[4])
    def _():
        fbuf[1 + co, x, my_rows, :] = sbuf[1]

    remote(sbuf.at[2], sbuf.at[2], s_send.at[1], s_recv.at[1], z=up).wait_recv()
    for step in (2, 1, 3):
        to_holder(2, 7 + step, step, jnp.int32(HOLDER[step + 4]), yh + step >= YH)
    to_holder(2, 7, 0, jnp.int32(HOLDER[0]), jnp.logical_and(co == 1, jnp.logical_not(is_root)))

    @pl.when(jnp.logical_and(is_root, co == 1))
    def _():
        fbuf[2, x, my_rows, :] = sbuf[2]

    own_first = jnp.logical_and(is_root, co == 0)
    kind = jnp.where(own_first, 0, 1)
    source = jnp.where(own_first, 0, 1 + co)
    here = jnp.logical_or(is_root, rep == HOLDER[4])

    def block_of(slot, origin):
        return fbuf.at[slot, lax.rem(origin, X), pl.ds(pl.multiple_of(origin // X * 128, 128), 128)]

    def pass_on(t, _):
        origin = lax.rem(rep + t, 8)

        known = jnp.logical_or(jnp.logical_and(origin == rep, here), jnp.logical_and(origin == twin, own_first))

        @pl.when(jnp.logical_not(known))
        def _():
            remote(
                block_of(source, origin), block_of(source, origin), f_send.at[0], f_recv.at[kind, origin],
                co=1 - co,
            ).wait_recv()

        remote(
            block_of(source, origin), block_of(1 + co, origin), d_send.at[origin], d_recv.at[origin], co=1 - co
        ).start()
        return 0

    lax.fori_loop(0, 8, pass_on, 0)

    def own_arrived(t, _):
        origin = lax.rem(rep + t, 8)

        @pl.when(origin != twin)
        def _():
            remote(
                block_of(0, origin), block_of(0, origin), f_send.at[0], f_recv.at[0, origin], co=1 - co
            ).wait_recv()

        return 0

    @pl.when(jnp.logical_not(own_first))
    def _():
        lax.fori_loop(1, 8, own_arrived, 0)

    for core in range(CO):
        expected = jnp.logical_or(jnp.logical_not(is_root), co != core)

        @pl.when(expected)
        def _(core=core):
            remote(esend, ebuf.at[core], e_send.at[0], e_recv.at[core], co=1 - co).wait_recv()

    virt_copy.wait()
    row = jnp.broadcast_to(virt_v[...], (256, 256))
    spread = row + row.T - occ_ref[0]

    def pair(order):
        which = co if order == 0 else 1 - co
        slot = jnp.where(jnp.logical_and(is_root, co == which), 0, 1 + which)
        coulomb = jnp.zeros((256, 256), F32)
        for xx in range(X):
            ih, il = halves(fbuf[0, xx])
            jh, jl = halves(fbuf[slot, xx])
            jhi[order, xx] = jh
            jlo[order, xx] = jl
            coulomb = coulomb + (mm_nt(ih, jh) + (mm_nt(ih, jl) + mm_nt(il, jh)))
        amplitude = (2.0 * coulomb - coulomb.T) / (spread - ebuf[which][0:1, 0:1])
        th, tl = halves(amplitude)
        thi[order] = th
        tlo[order] = tl

    pair(0)

    def twin_arrived(t, _):
        remote(
            block_of(2 - co, t), block_of(2 - co, t), d_send.at[t], d_recv.at[t], co=1 - co
        ).wait_recv()
        return 0

    lax.fori_loop(0, 8, twin_arrived, 0)
    pair(1)

    for step in (2, 1, 3, 0):
        xx = lax.rem(x + step, X)
        block = jnp.zeros((256, 256), F32)
        for order in range(2):
            block = block + mm3((thi[order], tlo[order]), (jhi[order, xx], jlo[order, xx]))
        for half in range(YL):
            g[xx, half] = block[:, half * NQ : (half + 1) * NQ]
        if step:
            for half in range(YL):
                launch(
                    remote(
                        g.at[xx, half], grecv.at[rep], g_send.at[YL * step + half], g_recv.at[rep],
                        yl=jnp.int32(half), x=xx,
                    )
                )
        else:
            launch(
                remote(g.at[xx, 1 - yl], grecv.at[rep], g_send.at[0], g_recv.at[rep], yl=1 - yl, x=xx)
            )
            grecv[rep] = g[xx, yl]

    def gradient_arrived(t, _):
        origin = lax.rem(rep + t, 8)
        remote(grecv.at[origin], grecv.at[origin], g_send.at[0], g_recv.at[origin], co=1 - co).wait_recv()
        return 0

    lax.fori_loop(1, 8, gradient_arrived, 0)
    result = grecv[0]
    for origin in range(1, 8):
        result = result + grecv[origin]
    out_ref[...] = result

    remote(
        hsend.at[pl.ds(0, NI - 1)], hx.at[x, pl.ds(0, NI - 1)], a2a_send, a2a_recv, co=1 - co
    ).wait_send()
    for copy in metric + gathers:
        copy.wait_send()
    for when, copy in energies:
        @pl.when(when)
        def _(copy=copy):
            copy.wait_send()
    for copy, when in sends:
        if when is None:
            copy.wait_send()
        else:
            @pl.when(when)
            def _(copy=copy):
                copy.wait_send()

    def passed(t, _):
        remote(
            block_of(source, t), block_of(1 + co, t), d_send.at[t], d_recv.at[t], co=1 - co
        ).wait_send()
        return 0

    lax.fori_loop(0, 8, passed, 0)


def per_device(raw_integrals, virtual_coeffs, metric_root, occ_energies, virt_energies):
    vmem = pl.BlockSpec(memory_space=pltpu.VMEM)
    anywhere = pl.BlockSpec(memory_space=pl.ANY)
    dma = pltpu.SemaphoreType.DMA
    out = pl.pallas_call(
        kernel,
        out_shape=jax.ShapeDtypeStruct((256, NQ), F32),
        in_specs=[anywhere, anywhere, anywhere, pl.BlockSpec(memory_space=pltpu.SMEM), anywhere],
        out_specs=vmem,
        scratch_shapes=[
            pltpu.VMEM((4, NI * NP, 128), F32),
            pltpu.VMEM((NA, NM), F32),
            pltpu.VMEM((1, 256), F32),
            pltpu.VMEM((YL, 1024, NQ), F32),
            pltpu.VMEM((NI, 4, 128), F32),
            pltpu.VMEM((X, NI, 4, 128), F32),
            pltpu.VMEM((3, 128, 256), F32),
            pltpu.VMEM((3, X, 256, 256), F32),
            pltpu.VMEM((2, X, 256, 256), BF16),
            pltpu.VMEM((2, X, 256, 256), BF16),
            pltpu.VMEM((2, 256, 256), BF16),
            pltpu.VMEM((2, 256, 256), BF16),
            pltpu.VMEM((8, 128), F32),
            pltpu.VMEM((2, 8, 128), F32),
            pltpu.VMEM((X, YL, 256, NQ), F32),
            pltpu.VMEM((8, 256, NQ), F32),
            dma((7,)), dma, dma, dma((2,)), dma((2,)), dma((2,)), dma((2,)), dma((4,)), dma((4,)),
            dma((2,)), dma((2,)), dma((8,)), dma((2, 8)), dma((11,)), dma((8,)), dma((8,)), dma((8,)), dma((8,)),
        ],
        compiler_params=pltpu.CompilerParams(
            collective_id=0, has_side_effects=True, vmem_limit_bytes=67043328
        ),
        name="gradient_density",
    )(
        raw_integrals.reshape(NI * NP, NM), virtual_coeffs.T, metric_root,
        occ_energies, virt_energies.reshape(1, 256),
    )
    return out[None]


def solution(mesh):
    finer = Mesh(mesh.devices.reshape(Z, YH, CO, YL, X), BLK + REP)
    return jax.shard_map(
        per_device,
        mesh=finer,
        in_specs=(P(None, BLK, None), P(None, REP), P(None, REP), P(BLK), P()),
        out_specs=P(BLK, None, REP),
        check_vma=False,
    )
```

```python
import jax
import jax.numpy as jnp
from jax import lax
from jax.experimental import pallas as pl
from jax.experimental.pallas import tpu as pltpu
from jax.sharding import Mesh
from jax.sharding import PartitionSpec as P

F32 = jnp.float32
BF16 = jnp.bfloat16
MESH = pl.DeviceIdType.MESH
Z, YH, CO, YL, X = 8, 4, 2, 2, 4
BLK = ("z", "yh", "co")
REP = ("yl", "x")
NI, NP, NM, NA, NQ = 64, 16, 512, 32, 128
DISTANCE = (1, 5, 2, 0, 3, 7, 6, 4)


def halves(v):
    high = v.astype(BF16)
    return high, (v - high.astype(F32)).astype(BF16)


def mm(a, b):
    return jnp.dot(a, b, preferred_element_type=F32)


def mm3(a, b):
    return mm(a[0], b[0]) + (mm(a[0], b[1]) + mm(a[1], b[0]))


def mm_nt(a, b):
    return lax.dot_general(a, b, (((1,), (1,)), ((), ())), preferred_element_type=F32)


def strided(ref, count, k):
    parts = []
    for part in range(count):
        rows = [ref[part, pl.ds(4 * p + k, NI, stride=NP), :] for p in range(4)]
        parts.append(jnp.concatenate(rows, axis=0))
    return jnp.concatenate(parts, axis=1)


def pick(index, table):
    out = table[-1]
    for at in range(len(table) - 2, -1, -1):
        out = jnp.where(index == at, table[at], out)
    return jnp.int32(out)


def kernel(
    raw_hbm, c_hbm, m_hbm, occ_ref, virt_hbm, out_ref,
    raw_v, c_v, virt_v, mbuf, hsend, hx, sbuf, rbuf, fbuf, jhi, jlo, thi, tlo, esend, ebuf, g, grecv,
    local_sem, a2a_send, a2a_recv, m_send, m_recv, e_send, e_recv, x_send, x_recv,
    s_send, s_recv, f_send, f_recv, p_send, r_recv, c_send, q_send, d_send, d_recv, g_send, g_recv,
):
    z, yh, co = lax.axis_index("z"), lax.axis_index("yh"), lax.axis_index("co")
    yl, x = lax.axis_index("yl"), lax.axis_index("x")
    me = (z * YH + yh) * CO + co
    chip = z * YH + yh
    rep = yl * X + x
    is_root = jnp.logical_and(yl == 0, x == 3)

    def remote(src, dst, ss, rs, **where):
        return pltpu.make_async_remote_copy(
            src_ref=src, dst_ref=dst, send_sem=ss, recv_sem=rs, device_id=where, device_id_type=MESH
        )

    c_copy = pltpu.make_async_copy(c_hbm, c_v, local_sem.at[5])
    c_copy.start()
    raw_copies = []
    for part in range(4):
        raw_copies.append(
            pltpu.make_async_copy(raw_hbm.at[:, pl.ds(128 * part, 128)], raw_v.at[part], local_sem.at[1 + part])
        )
        raw_copies[-1].start()
    m_copy = pltpu.make_async_copy(m_hbm, mbuf.at[yl], local_sem.at[0])
    m_copy.start()
    virt_copy = pltpu.make_async_copy(virt_hbm, virt_v, local_sem.at[6])
    virt_copy.start()

    zs = [lax.rem(z + step, Z) for step in range(Z)]
    yhs = [lax.rem(yh + step, YH) for step in range(YH)]
    cos = [co, 1 - co]
    yls = [yl, 1 - yl]
    xs = [lax.rem(x + step, X) for step in range(X)]
    across_blk = [(a, b, c) for a in (4, 3, 5, 2, 6, 1, 7, 0) for b in (2, 1, 3, 0) for c in (0, 1)][:-2] + [(0, 0, 1)]
    across_plane = [(a, b, c) for a in (2, 1, 3, 0) for b in (0, 1) for c in (2, 1, 3, 0) if (b, c) != (0, 0)]

    barrier = pltpu.get_barrier_semaphore()
    for a, b, c in across_blk:
        pl.semaphore_signal(
            barrier, inc=1, device_id={"z": zs[a], "yh": yhs[b], "co": cos[c]}, device_id_type=MESH
        )
    for a, b, c in across_plane:
        pl.semaphore_signal(
            barrier, inc=1, device_id={"yh": yhs[a], "yl": yls[b], "x": xs[c]}, device_id_type=MESH
        )

    esend[...] = jnp.full((8, 128), occ_ref[0], F32)

    c_copy.wait()
    c_high, c_low = halves(c_v[...].T)
    for copy in raw_copies:
        copy.wait()
    total = jnp.zeros((4 * NI, 128), F32)
    for k in range(4):
        place = (
            lax.broadcasted_iota(jnp.int32, (NA, 128), 1) == lax.broadcasted_iota(jnp.int32, (NA, 128), 0) + NA * k
        ).astype(F32).astype(BF16)
        right = (mm(c_high, place).astype(BF16), mm(c_low, place).astype(BF16))
        rows = strided(raw_v, 4, k)
        total = total + mm3(halves(rows), right)
    for p in range(4):
        hsend[:, p, :] = total[NI * p : NI * (p + 1)]

    pl.semaphore_wait(barrier, len(across_blk) + len(across_plane))

    for a, b, c in across_blk:
        other = (zs[a] * YH + yhs[b]) * CO + cos[c]
        remote(hsend.at[other], hx.at[x, me], a2a_send, a2a_recv, z=zs[a], yh=yhs[b], co=cos[c]).start()
    hx[x, me] = hsend[me]

    y = yh * YL + yl
    metric = []
    for side, to in ((0, lax.rem(y + 1, 8)), (1, lax.rem(y + 7, 8))):
        rows_of = pl.ds(side * 512, 512)
        copy = remote(
            m_hbm.at[rows_of], mbuf.at[yl, rows_of], m_send.at[side], m_recv.at[side],
            yh=to // YL, yl=lax.rem(to, YL),
        )
        copy.start()
        metric.append(copy)

    distance = pick(rep, DISTANCE)
    ahead = chip + distance
    energies = []
    for core in range(CO):
        energies.append((
            jnp.logical_not(is_root),
            remote(
                esend, ebuf.at[co], e_send.at[core], e_recv.at[co],
                z=lax.rem(ahead // YH, Z), yh=lax.rem(ahead, YH), co=jnp.int32(core),
            ),
        ))
    energies.append((
        jnp.logical_and(is_root, co == 1),
        remote(esend, ebuf.at[1], e_send.at[0], e_recv.at[1], z=lax.rem(z + 2, Z), co=jnp.int32(0)),
    ))
    energies.append((
        jnp.logical_and(is_root, co == 0),
        remote(esend, ebuf.at[0], e_send.at[0], e_recv.at[0], co=jnp.int32(1)),
    ))
    for when, copy in energies:
        @pl.when(when)
        def _(copy=copy):
            copy.start()

    @pl.when(is_root)
    def _():
        ebuf[co] = esend[...]

    remote(
        hx.at[x, pl.ds(0, NI - 1)], hx.at[x, pl.ds(0, NI - 1)], a2a_send, a2a_recv, co=1 - co
    ).wait_recv()
    gathers = []
    for step in (2, 1, 3):
        copy = remote(hx.at[x], hx.at[x], x_send.at[step], x_recv.at[x], x=lax.rem(x + step, X))
        copy.start()
        gathers.append(copy)
    m_copy.wait()
    for copy in metric:
        copy.wait_recv()
    for step in (1, 3, 2):
        origin = lax.rem(x + step, X)
        remote(hx.at[origin], hx.at[origin], x_send.at[step], x_recv.at[origin], x=origin).wait_recv()

    turned = []
    for xx in range(X):
        block = jnp.concatenate([hx[xx, :, p, :] for p in range(4)], axis=0)
        turned.append(block.T)
    part = jnp.zeros((128, 256), F32)
    for k in range(4):
        left = jnp.concatenate([t[NA * k : NA * (k + 1), :] for t in turned], axis=0)
        right = strided(mbuf, 2, k)
        part = part + mm3(halves(left), halves(right))
    my_rows = pl.ds(pl.multiple_of(yl * 128, 128), 128)
    sbuf[0] = part
    fbuf[0, x, my_rows, :] = part

    up = zs[1]
    sends = []

    def launch(copy, when=None):
        sends.append((copy, when))
        if when is None:
            copy.start()
        else:
            @pl.when(when)
            def _():
                copy.start()

    wraps = {1: yh == YH - 1, 3: yh > 0}

    def to_edge(slot, index, step, k, when=None):
        launch(
            remote(
                sbuf.at[slot], rbuf.at[k, yl], p_send.at[index], r_recv.at[k, yl],
                yh=yhs[step], yl=jnp.int32(step // 2),
            ),
            when,
        )

    def gather_row(origin_rows, origin, index):
        for step in (2, 1, 3):
            launch(
                remote(
                    fbuf.at[0, x, origin_rows], fbuf.at[0, x, origin_rows], f_send.at[index + step],
                    f_recv.at[0, origin], x=xs[step],
                )
            )

    other_rows = pl.ds(pl.multiple_of((1 - yl) * 128, 128), 128)
    twin = (1 - yl) * X + x
    launch(remote(sbuf.at[0], sbuf.at[1], s_send.at[0], s_recv.at[0], z=up))
    launch(remote(sbuf.at[0], fbuf.at[0, x, my_rows], f_send.at[0], f_recv.at[0, rep], yl=1 - yl))
    for step in (1, 3):
        to_edge(0, step // 2, step, 0, jnp.logical_not(wraps[step]))
    gather_row(my_rows, rep, 0)
    remote(
        fbuf.at[0, x, other_rows], fbuf.at[0, x, other_rows], f_send.at[0], f_recv.at[0, twin], co=1 - co
    ).wait_recv()
    gather_row(other_rows, twin, 4)

    remote(sbuf.at[1], sbuf.at[1], s_send.at[0], s_recv.at[0], z=up).wait_recv()
    launch(remote(sbuf.at[1], sbuf.at[2], s_send.at[1], s_recv.at[1], z=up))
    for step in (1, 3):
        to_edge(1, 2 + step // 2, step, jnp.where(wraps[step], 0, 1))
    launch(remote(sbuf.at[1], rbuf.at[3, 0], p_send.at[6], r_recv.at[3, 0], yl=jnp.int32(1)), yl == 0)

    goes_on = jnp.where(yl == 0, jnp.where(yh == YH - 1, 1, 0), jnp.where(yh == 0, 0, 1))
    onward = jnp.where(yl == 0, yhs[1], yhs[3])

    def deliver(src, k, row, when=None):
        rows = pl.ds(row * 128, 128) if isinstance(row, int) else pl.ds(pl.multiple_of(row * 128, 128), 128)
        away = x != k if when is None else jnp.logical_and(x != k, when)
        launch(
            remote(
                src, fbuf.at[1 + co, x, rows], q_send.at[k, row], f_recv.at[1, row * X + x], x=jnp.int32(k)
            ),
            away,
        )

        @pl.when(x == k if when is None else jnp.logical_and(x == k, when))
        def _():
            fbuf[1 + co, x, rows, :] = src[...]

    def arrived(k, row):
        return remote(rbuf.at[k, row], rbuf.at[k, row], q_send.at[0, 0], r_recv.at[k, row], co=1 - co)

    def relay(k):
        for row in range(YL):
            arrived(k, row).wait_recv()
            if k < 2:
                launch(
                    remote(rbuf.at[k, row], rbuf.at[2, row], c_send.at[k, row], r_recv.at[2, row], yh=onward),
                    goes_on == k,
                )
            deliver(rbuf.at[k, row], k, row)

    relay(0)
    remote(sbuf.at[2], sbuf.at[2], s_send.at[1], s_recv.at[1], z=up).wait_recv()
    for step in (1, 3):
        to_edge(2, 4 + step // 2, step, 1, wraps[step])
    last = jnp.logical_and(yl == 1, co == 1)
    launch(remote(sbuf.at[2], rbuf.at[3, 1], p_send.at[7], r_recv.at[3, 1], yl=jnp.int32(0)), last)
    relay(1)

    takes = jnp.logical_or(yl == 1, co == 1)

    @pl.when(takes)
    def _():
        arrived(3, 1 - yl).wait_recv()

    deliver(rbuf.at[3, 1 - yl], 3, 1 - yl, takes)
    deliver(sbuf.at[2 - yl], 3, yl, takes)
    relay(2)

    own_first = jnp.logical_and(is_root, co == 0)
    kind = jnp.where(own_first, 0, 1)
    source = jnp.where(own_first, 0, 1 + co)

    def block_of(slot, origin):
        return fbuf.at[slot, lax.rem(origin, X), pl.ds(pl.multiple_of(origin // X * 128, 128), 128)]

    def pass_on(t, _):
        origin = lax.rem(rep + t, 8)

        known = lax.rem(origin, X) == x

        @pl.when(jnp.logical_not(known))
        def _():
            remote(
                block_of(source, origin), block_of(source, origin), f_send.at[0], f_recv.at[kind, origin],
                co=1 - co,
            ).wait_recv()

        remote(
            block_of(source, origin), block_of(1 + co, origin), d_send.at[origin], d_recv.at[origin], co=1 - co
        ).start()
        return 0

    lax.fori_loop(0, 8, pass_on, 0)

    def own_arrived(t, _):
        origin = lax.rem(rep + t, 8)

        @pl.when(origin != twin)
        def _():
            remote(
                block_of(0, origin), block_of(0, origin), f_send.at[0], f_recv.at[0, origin], co=1 - co
            ).wait_recv()

        return 0

    @pl.when(jnp.logical_not(own_first))
    def _():
        lax.fori_loop(1, 8, own_arrived, 0)

    for core in range(CO):
        expected = jnp.logical_or(jnp.logical_not(is_root), co != core)

        @pl.when(expected)
        def _(core=core):
            remote(esend, ebuf.at[core], e_send.at[0], e_recv.at[core], co=1 - co).wait_recv()

    virt_copy.wait()
    row = jnp.broadcast_to(virt_v[...], (256, 256))
    spread = row + row.T - occ_ref[0]

    def pair(order):
        which = co if order == 0 else 1 - co
        slot = jnp.where(jnp.logical_and(is_root, co == which), 0, 1 + which)
        coulomb = jnp.zeros((256, 256), F32)
        for xx in range(X):
            ih, il = halves(fbuf[0, xx])
            jh, jl = halves(fbuf[slot, xx])
            jhi[order, xx] = jh
            jlo[order, xx] = jl
            coulomb = coulomb + (mm_nt(ih, jh) + (mm_nt(ih, jl) + mm_nt(il, jh)))
        amplitude = (2.0 * coulomb - coulomb.T) / (spread - ebuf[which][0:1, 0:1])
        th, tl = halves(amplitude)
        thi[order] = th
        tlo[order] = tl

    pair(0)

    def twin_arrived(t, _):
        remote(
            block_of(2 - co, t), block_of(2 - co, t), d_send.at[t], d_recv.at[t], co=1 - co
        ).wait_recv()
        return 0

    lax.fori_loop(0, 8, twin_arrived, 0)
    pair(1)

    for step in (2, 1, 3, 0):
        xx = lax.rem(x + step, X)
        block = jnp.zeros((256, 256), F32)
        for order in range(2):
            block = block + mm3((thi[order], tlo[order]), (jhi[order, xx], jlo[order, xx]))
        for half in range(YL):
            g[xx, half] = block[:, half * NQ : (half + 1) * NQ]
        if step:
            for half in range(YL):
                launch(
                    remote(
                        g.at[xx, half], grecv.at[rep], g_send.at[YL * step + half], g_recv.at[rep],
                        yl=jnp.int32(half), x=xx,
                    )
                )
        else:
            launch(
                remote(g.at[xx, 1 - yl], grecv.at[rep], g_send.at[0], g_recv.at[rep], yl=1 - yl, x=xx)
            )
            grecv[rep] = g[xx, yl]

    def gradient_arrived(t, _):
        origin = lax.rem(rep + t, 8)
        remote(grecv.at[origin], grecv.at[origin], g_send.at[0], g_recv.at[origin], co=1 - co).wait_recv()
        return 0

    lax.fori_loop(1, 8, gradient_arrived, 0)
    result = grecv[0]
    for origin in range(1, 8):
        result = result + grecv[origin]
    out_ref[...] = result

    remote(
        hsend.at[pl.ds(0, NI - 1)], hx.at[x, pl.ds(0, NI - 1)], a2a_send, a2a_recv, co=1 - co
    ).wait_send()
    for copy in metric + gathers:
        copy.wait_send()
    for when, copy in energies:
        @pl.when(when)
        def _(copy=copy):
            copy.wait_send()
    for copy, when in sends:
        if when is None:
            copy.wait_send()
        else:
            @pl.when(when)
            def _(copy=copy):
                copy.wait_send()

    def passed(t, _):
        remote(
            block_of(source, t), block_of(1 + co, t), d_send.at[t], d_recv.at[t], co=1 - co
        ).wait_send()
        return 0

    lax.fori_loop(0, 8, passed, 0)


def per_device(raw_integrals, virtual_coeffs, metric_root, occ_energies, virt_energies):
    vmem = pl.BlockSpec(memory_space=pltpu.VMEM)
    anywhere = pl.BlockSpec(memory_space=pl.ANY)
    dma = pltpu.SemaphoreType.DMA
    out = pl.pallas_call(
        kernel,
        out_shape=jax.ShapeDtypeStruct((256, NQ), F32),
        in_specs=[anywhere, anywhere, anywhere, pl.BlockSpec(memory_space=pltpu.SMEM), anywhere],
        out_specs=vmem,
        scratch_shapes=[
            pltpu.VMEM((4, NI * NP, 128), F32),
            pltpu.VMEM((NA, NM), F32),
            pltpu.VMEM((1, 256), F32),
            pltpu.VMEM((YL, 1024, NQ), F32),
            pltpu.VMEM((NI, 4, 128), F32),
            pltpu.VMEM((X, NI, 4, 128), F32),
            pltpu.VMEM((3, 128, 256), F32),
            pltpu.VMEM((4, YL, 128, 256), F32),
            pltpu.VMEM((3, X, 256, 256), F32),
            pltpu.VMEM((2, X, 256, 256), BF16),
            pltpu.VMEM((2, X, 256, 256), BF16),
            pltpu.VMEM((2, 256, 256), BF16),
            pltpu.VMEM((2, 256, 256), BF16),
            pltpu.VMEM((8, 128), F32),
            pltpu.VMEM((2, 8, 128), F32),
            pltpu.VMEM((X, YL, 256, NQ), F32),
            pltpu.VMEM((8, 256, NQ), F32),
            dma((7,)), dma, dma, dma((2,)), dma((2,)), dma((2,)), dma((2,)), dma((4,)), dma((4,)),
            dma((2,)), dma((2,)), dma((8,)), dma((2, 8)),
            dma((8,)), dma((4, 2)), dma((2, 2)), dma((4, 2)), dma((8,)), dma((8,)), dma((8,)), dma((8,)),
        ],
        compiler_params=pltpu.CompilerParams(
            collective_id=0, has_side_effects=True, vmem_limit_bytes=67043328
        ),
        name="gradient_density",
    )(
        raw_integrals.reshape(NI * NP, NM), virtual_coeffs.T, metric_root,
        occ_energies, virt_energies.reshape(1, 256),
    )
    return out[None]


def solution(mesh):
    finer = Mesh(mesh.devices.reshape(Z, YH, CO, YL, X), BLK + REP)
    return jax.shard_map(
        per_device,
        mesh=finer,
        in_specs=(P(None, BLK, None), P(None, REP), P(None, REP), P(BLK), P()),
        out_specs=P(BLK, None, REP),
        check_vma=False,
    )
```

```python
import jax
import jax.numpy as jnp
from jax import lax
from jax.experimental import pallas as pl
from jax.experimental.pallas import tpu as pltpu
from jax.sharding import Mesh
from jax.sharding import PartitionSpec as P

F32 = jnp.float32
BF16 = jnp.bfloat16
MESH = pl.DeviceIdType.MESH
Z, YH, CO, YL, X = 8, 4, 2, 2, 4
BLK = ("z", "yh", "co")
REP = ("yl", "x")
NI, NP, NM, NA, NQ = 64, 16, 512, 32, 128
HOLDER = (1, 2, 0, 6, 4, 3, 5, 7)
DISTANCE = (2, 0, 1, 5, 4, 6, 3, 7)


def halves(v):
    high = v.astype(BF16)
    return high, (v - high.astype(F32)).astype(BF16)


def mm(a, b):
    return jnp.dot(a, b, preferred_element_type=F32)


def mm3(a, b):
    return mm(a[0], b[0]) + (mm(a[0], b[1]) + mm(a[1], b[0]))


def mm_nt(a, b):
    return lax.dot_general(a, b, (((1,), (1,)), ((), ())), preferred_element_type=F32)


def strided(ref, count, k):
    parts = []
    for part in range(count):
        rows = [ref[part, pl.ds(4 * p + k, NI, stride=NP), :] for p in range(4)]
        parts.append(jnp.concatenate(rows, axis=0))
    return jnp.concatenate(parts, axis=1)


def pick(index, table):
    out = table[-1]
    for at in range(len(table) - 2, -1, -1):
        out = jnp.where(index == at, table[at], out)
    return jnp.int32(out)


def kernel(
    raw_hbm, c_hbm, m_hbm, occ_ref, virt_hbm, out_ref,
    raw_v, c_v, virt_v, mbuf, hsend, hx, sbuf, fbuf, jhi, jlo, thi, tlo, esend, ebuf, g, grecv, tbuf,
    local_sem, a2a_send, a2a_recv, m_send, m_recv, e_send, e_recv, x_send, x_recv,
    s_send, s_recv, f_send, f_recv, p_send, d_send, d_recv, g_send, g_recv,
):
    z, yh, co = lax.axis_index("z"), lax.axis_index("yh"), lax.axis_index("co")
    yl, x = lax.axis_index("yl"), lax.axis_index("x")
    me = (z * YH + yh) * CO + co
    chip = z * YH + yh
    rep = yl * X + x
    is_root = rep == HOLDER[0]

    def remote(src, dst, ss, rs, **where):
        return pltpu.make_async_remote_copy(
            src_ref=src, dst_ref=dst, send_sem=ss, recv_sem=rs, device_id=where, device_id_type=MESH
        )

    c_copy = pltpu.make_async_copy(c_hbm, c_v, local_sem.at[5])
    c_copy.start()
    raw_copies = []
    for part in range(4):
        raw_copies.append(
            pltpu.make_async_copy(raw_hbm.at[:, pl.ds(128 * part, 128)], raw_v.at[part], local_sem.at[1 + part])
        )
        raw_copies[-1].start()
    m_copy = pltpu.make_async_copy(m_hbm, mbuf.at[yl], local_sem.at[0])
    m_copy.start()
    virt_copy = pltpu.make_async_copy(virt_hbm, virt_v, local_sem.at[6])
    virt_copy.start()

    zs = [lax.rem(z + step, Z) for step in range(Z)]
    yhs = [lax.rem(yh + step, YH) for step in range(YH)]
    cos = [co, 1 - co]
    yls = [yl, 1 - yl]
    xs = [lax.rem(x + step, X) for step in range(X)]
    across_blk = [(a, b, c) for a in (4, 3, 5, 2, 6, 1, 7, 0) for b in (2, 1, 3, 0) for c in (0, 1)][:-2] + [(0, 0, 1)]
    across_plane = [(a, b, c) for a in (2, 1, 3, 0) for b in (0, 1) for c in (2, 1, 3, 0) if (b, c) != (0, 0)]

    barrier = pltpu.get_barrier_semaphore()
    for a, b, c in across_blk:
        pl.semaphore_signal(
            barrier, inc=1, device_id={"z": zs[a], "yh": yhs[b], "co": cos[c]}, device_id_type=MESH
        )
    for a, b, c in across_plane:
        pl.semaphore_signal(
            barrier, inc=1, device_id={"yh": yhs[a], "yl": yls[b], "x": xs[c]}, device_id_type=MESH
        )

    esend[...] = jnp.full((8, 128), occ_ref[0], F32)

    c_copy.wait()
    c_high, c_low = halves(c_v[...].T)
    for copy in raw_copies:
        copy.wait()
    total = jnp.zeros((4 * NI, 128), F32)
    for k in range(4):
        place = (
            lax.broadcasted_iota(jnp.int32, (NA, 128), 1) == lax.broadcasted_iota(jnp.int32, (NA, 128), 0) + NA * k
        ).astype(F32).astype(BF16)
        right = (mm(c_high, place).astype(BF16), mm(c_low, place).astype(BF16))
        rows = strided(raw_v, 4, k)
        total = total + mm3(halves(rows), right)
    for p in range(4):
        hsend[:, p, :] = total[NI * p : NI * (p + 1)]

    pl.semaphore_wait(barrier, len(across_blk) + len(across_plane))

    for a, b, c in across_blk:
        other = (zs[a] * YH + yhs[b]) * CO + cos[c]
        remote(hsend.at[other], hx.at[x, me], a2a_send, a2a_recv, z=zs[a], yh=yhs[b], co=cos[c]).start()
    hx[x, me] = hsend[me]

    y = yh * YL + yl
    metric = []
    for side, to in ((0, lax.rem(y + 1, 8)), (1, lax.rem(y + 7, 8))):
        rows_of = pl.ds(side * 512, 512)
        copy = remote(
            m_hbm.at[rows_of], mbuf.at[yl, rows_of], m_send.at[side], m_recv.at[side],
            yh=to // YL, yl=lax.rem(to, YL),
        )
        copy.start()
        metric.append(copy)

    distance = pick(rep, DISTANCE)
    ahead = chip + distance
    energies = []
    for core in range(CO):
        energies.append((
            jnp.logical_not(is_root),
            remote(
                esend, ebuf.at[co], e_send.at[core], e_recv.at[co],
                z=lax.rem(ahead // YH, Z), yh=lax.rem(ahead, YH), co=jnp.int32(core),
            ),
        ))
    energies.append((
        jnp.logical_and(is_root, co == 1),
        remote(esend, ebuf.at[1], e_send.at[0], e_recv.at[1], z=lax.rem(z + 2, Z), co=jnp.int32(0)),
    ))
    energies.append((
        jnp.logical_and(is_root, co == 0),
        remote(esend, ebuf.at[0], e_send.at[0], e_recv.at[0], co=jnp.int32(1)),
    ))
    for when, copy in energies:
        @pl.when(when)
        def _(copy=copy):
            copy.start()

    @pl.when(is_root)
    def _():
        ebuf[co] = esend[...]

    remote(
        hx.at[x, pl.ds(0, NI - 1)], hx.at[x, pl.ds(0, NI - 1)], a2a_send, a2a_recv, co=1 - co
    ).wait_recv()
    gathers = []
    for step in (2, 1, 3):
        copy = remote(hx.at[x], hx.at[x], x_send.at[step], x_recv.at[x], x=lax.rem(x + step, X))
        copy.start()
        gathers.append(copy)
    m_copy.wait()
    for copy in metric:
        copy.wait_recv()
    for step in (1, 3, 2):
        origin = lax.rem(x + step, X)
        remote(hx.at[origin], hx.at[origin], x_send.at[step], x_recv.at[origin], x=origin).wait_recv()

    turned = []
    for xx in range(X):
        block = jnp.concatenate([hx[xx, :, p, :] for p in range(4)], axis=0)
        turned.append(block.T)
    part = jnp.zeros((128, 256), F32)
    for k in range(4):
        left = jnp.concatenate([t[NA * k : NA * (k + 1), :] for t in turned], axis=0)
        right = strided(mbuf, 2, k)
        part = part + mm3(halves(left), halves(right))
    my_rows = pl.ds(pl.multiple_of(yl * 128, 128), 128)
    sbuf[0] = part
    fbuf[0, x, my_rows, :] = part

    up = lax.rem(z + 1, Z)
    sends = []

    def launch(copy, when=None):
        sends.append((copy, when))
        if when is None:
            copy.start()
        else:
            @pl.when(when)
            def _():
                copy.start()

    def to_holder(slot, index, steps, holder, when=None):
        launch(
            remote(
                sbuf.at[slot], fbuf.at[1 + co, x, my_rows], p_send.at[index], f_recv.at[1, rep],
                yh=lax.rem(yh + steps, YH), yl=holder // X, x=lax.rem(holder, X),
            ),
            when,
        )

    launch(remote(sbuf.at[0], sbuf.at[1], s_send.at[0], s_recv.at[0], z=up))
    for step in range(1, 4):
        to_holder(0, step - 1, step, jnp.int32(HOLDER[step]), yh + step < YH)
    other_rows = pl.ds(pl.multiple_of((1 - yl) * 128, 128), 128)
    twin = (1 - yl) * X + x
    launch(
        remote(
            fbuf.at[0, x, my_rows], fbuf.at[0, x, my_rows], f_send.at[0], f_recv.at[0, rep], yl=1 - yl
        )
    )
    for step in (2, 1, 3):
        launch(
            remote(
                fbuf.at[0, x, my_rows], fbuf.at[0, x, my_rows], f_send.at[step], f_recv.at[0, rep], x=xs[step]
            )
        )
    remote(
        fbuf.at[0, x, other_rows], fbuf.at[0, x, other_rows], f_send.at[0], f_recv.at[0, twin], co=1 - co
    ).wait_recv()
    for step in (2, 1, 3):
        launch(
            remote(
                fbuf.at[0, x, other_rows], fbuf.at[0, x, other_rows], f_send.at[4 + step], f_recv.at[0, twin],
                x=xs[step],
            )
        )

    remote(sbuf.at[1], sbuf.at[1], s_send.at[0], s_recv.at[0], z=up).wait_recv()
    launch(remote(sbuf.at[1], sbuf.at[2], s_send.at[1], s_recv.at[1], z=up))
    for step in (2, 1, 3):
        holder = jnp.where(yh + step >= YH, HOLDER[step], HOLDER[step + 4])
        to_holder(1, 3 + step, step, holder)
    to_holder(1, 3, 0, jnp.int32(HOLDER[4]), rep != HOLDER[4])

    @pl.when(rep == HOLDER[4])
    def _():
        fbuf[1 + co, x, my_rows, :] = sbuf[1]

    remote(sbuf.at[2], sbuf.at[2], s_send.at[1], s_recv.at[1], z=up).wait_recv()
    for step in (2, 1, 3):
        to_holder(2, 7 + step, step, jnp.int32(HOLDER[step + 4]), yh + step >= YH)
    to_holder(2, 7, 0, jnp.int32(HOLDER[0]), jnp.logical_and(co == 1, jnp.logical_not(is_root)))

    @pl.when(jnp.logical_and(is_root, co == 1))
    def _():
        fbuf[2, x, my_rows, :] = sbuf[2]

    own_first = jnp.logical_and(is_root, co == 0)
    kind = jnp.where(own_first, 0, 1)
    source = jnp.where(own_first, 0, 1 + co)
    here = jnp.logical_or(is_root, rep == HOLDER[4])

    def block_of(slot, origin):
        return fbuf.at[slot, lax.rem(origin, X), pl.ds(pl.multiple_of(origin // X * 128, 128), 128)]

    def pass_on(t, _):
        origin = lax.rem(rep + t, 8)

        known = jnp.logical_or(jnp.logical_and(origin == rep, here), jnp.logical_and(origin == twin, own_first))

        @pl.when(jnp.logical_not(known))
        def _():
            remote(
                block_of(source, origin), block_of(source, origin), f_send.at[0], f_recv.at[kind, origin],
                co=1 - co,
            ).wait_recv()

        remote(
            block_of(source, origin), block_of(1 + co, origin), d_send.at[origin], d_recv.at[origin], co=1 - co
        ).start()
        return 0

    lax.fori_loop(0, 8, pass_on, 0)

    def own_arrived(t, _):
        origin = lax.rem(rep + t, 8)

        @pl.when(origin != twin)
        def _():
            remote(
                block_of(0, origin), block_of(0, origin), f_send.at[0], f_recv.at[0, origin], co=1 - co
            ).wait_recv()

        return 0

    @pl.when(jnp.logical_not(own_first))
    def _():
        lax.fori_loop(1, 8, own_arrived, 0)

    for core in range(CO):
        expected = jnp.logical_or(jnp.logical_not(is_root), co != core)

        @pl.when(expected)
        def _(core=core):
            remote(esend, ebuf.at[core], e_send.at[0], e_recv.at[core], co=1 - co).wait_recv()

    virt_copy.wait()
    row = jnp.broadcast_to(virt_v[...], (256, 256))
    spread = row + row.T - occ_ref[0]

    def pair(order):
        which = co if order == 0 else 1 - co
        slot = jnp.where(jnp.logical_and(is_root, co == which), 0, 1 + which)
        coulomb = jnp.zeros((256, 256), F32)
        for xx in range(X):
            ih, il = halves(fbuf[0, xx])
            jh, jl = halves(fbuf[slot, xx])
            jhi[order, xx] = jh
            jlo[order, xx] = jl
            coulomb = coulomb + (mm_nt(ih, jh) + (mm_nt(ih, jl) + mm_nt(il, jh)))
        amplitude = (2.0 * coulomb - coulomb.T) / (spread - ebuf[which][0:1, 0:1])
        th, tl = halves(amplitude)
        thi[order] = th
        tlo[order] = tl

    pair(0)

    def twin_arrived(t, _):
        remote(
            block_of(2 - co, t), block_of(2 - co, t), d_send.at[t], d_recv.at[t], co=1 - co
        ).wait_recv()
        return 0

    lax.fori_loop(0, 8, twin_arrived, 0)
    pair(1)

    def to_column(step, half, index):
        launch(
            remote(
                g.at[xs[step], half], grecv.at[x, half], g_send.at[step, index], g_recv.at[x, index], x=xs[step]
            )
        )

    for step in (2, 1, 3, 0):
        xx = xs[step]
        block = jnp.zeros((256, 256), F32)
        for order in range(2):
            block = block + mm3((thi[order], tlo[order]), (jhi[order, xx], jlo[order, xx]))
        for half in range(YL):
            g[xx, half] = block[:, half * NQ : (half + 1) * NQ]
        if step:
            to_column(step, 1 - yl, 0)
    for step in (2, 1, 3):
        to_column(step, yl, 1)

    def column_sum(half, index):
        for step in (1, 3, 2):
            block = grecv.at[xs[step], half]
            remote(block, block, g_send.at[0, 0], g_recv.at[xs[step], index], co=1 - co).wait_recv()
        result = g[x, half]
        for step in (1, 2, 3):
            result = result + grecv[xs[step], half]
        return result

    tbuf[0] = column_sum(1 - yl, 0)
    launch(remote(tbuf.at[0], tbuf.at[1], g_send.at[0, 0], g_recv.at[x, 0], yl=1 - yl))
    result = column_sum(yl, 1)
    remote(tbuf.at[1], tbuf.at[1], g_send.at[0, 0], g_recv.at[x, 0], co=1 - co).wait_recv()
    out_ref[...] = result + tbuf[1]

    remote(
        hsend.at[pl.ds(0, NI - 1)], hx.at[x, pl.ds(0, NI - 1)], a2a_send, a2a_recv, co=1 - co
    ).wait_send()
    for copy in metric + gathers:
        copy.wait_send()
    for when, copy in energies:
        @pl.when(when)
        def _(copy=copy):
            copy.wait_send()
    for copy, when in sends:
        if when is None:
            copy.wait_send()
        else:
            @pl.when(when)
            def _(copy=copy):
                copy.wait_send()

    def passed(t, _):
        remote(
            block_of(source, t), block_of(1 + co, t), d_send.at[t], d_recv.at[t], co=1 - co
        ).wait_send()
        return 0

    lax.fori_loop(0, 8, passed, 0)


def per_device(raw_integrals, virtual_coeffs, metric_root, occ_energies, virt_energies):
    vmem = pl.BlockSpec(memory_space=pltpu.VMEM)
    anywhere = pl.BlockSpec(memory_space=pl.ANY)
    dma = pltpu.SemaphoreType.DMA
    out = pl.pallas_call(
        kernel,
        out_shape=jax.ShapeDtypeStruct((256, NQ), F32),
        in_specs=[anywhere, anywhere, anywhere, pl.BlockSpec(memory_space=pltpu.SMEM), anywhere],
        out_specs=vmem,
        scratch_shapes=[
            pltpu.VMEM((4, NI * NP, 128), F32),
            pltpu.VMEM((NA, NM), F32),
            pltpu.VMEM((1, 256), F32),
            pltpu.VMEM((YL, 1024, NQ), F32),
            pltpu.VMEM((NI, 4, 128), F32),
            pltpu.VMEM((X, NI, 4, 128), F32),
            pltpu.VMEM((3, 128, 256), F32),
            pltpu.VMEM((3, X, 256, 256), F32),
            pltpu.VMEM((2, X, 256, 256), BF16),
            pltpu.VMEM((2, X, 256, 256), BF16),
            pltpu.VMEM((2, 256, 256), BF16),
            pltpu.VMEM((2, 256, 256), BF16),
            pltpu.VMEM((8, 128), F32),
            pltpu.VMEM((2, 8, 128), F32),
            pltpu.VMEM((X, YL, 256, NQ), F32),
            pltpu.VMEM((X, YL, 256, NQ), F32),
            pltpu.VMEM((2, 256, NQ), F32),
            dma((7,)), dma, dma, dma((2,)), dma((2,)), dma((2,)), dma((2,)), dma((4,)), dma((4,)),
            dma((2,)), dma((2,)), dma((8,)), dma((2, 8)), dma((11,)), dma((8,)), dma((8,)), dma((X, 2)), dma((X, 2)),
        ],
        compiler_params=pltpu.CompilerParams(
            collective_id=0, has_side_effects=True, vmem_limit_bytes=67043328
        ),
        name="gradient_density",
    )(
        raw_integrals.reshape(NI * NP, NM), virtual_coeffs.T, metric_root,
        occ_energies, virt_energies.reshape(1, 256),
    )
    return out[None]


def solution(mesh):
    finer = Mesh(mesh.devices.reshape(Z, YH, CO, YL, X), BLK + REP)
    return jax.shard_map(
        per_device,
        mesh=finer,
        in_specs=(P(None, BLK, None), P(None, REP), P(None, REP), P(BLK), P()),
        out_specs=P(BLK, None, REP),
        check_vma=False,
    )
```

```python
import jax
import jax.numpy as jnp
from jax import lax
from jax.experimental import pallas as pl
from jax.experimental.pallas import tpu as pltpu
from jax.sharding import Mesh
from jax.sharding import PartitionSpec as P

F32 = jnp.float32
BF16 = jnp.bfloat16
MESH = pl.DeviceIdType.MESH
Z, YH, CO, YL, X = 8, 4, 2, 2, 4
BLK = ("z", "yh", "co")
REP = ("yl", "x")
NI, NP, NM, NA, NQ = 64, 16, 512, 32, 128
HOLDER = (1, 2, 0, 6, 4, 3, 5, 7)
DISTANCE = (2, 0, 1, 5, 4, 6, 3, 7)


def halves(v):
    high = v.astype(BF16)
    return high, (v - high.astype(F32)).astype(BF16)


def mm(a, b):
    return jnp.dot(a, b, preferred_element_type=F32)


def mm3(a, b):
    return mm(a[0], b[0]) + (mm(a[0], b[1]) + mm(a[1], b[0]))


def mm_nt(a, b):
    return lax.dot_general(a, b, (((1,), (1,)), ((), ())), preferred_element_type=F32)


def strided(ref, count, k):
    parts = []
    for part in range(count):
        rows = [ref[part, pl.ds(4 * p + k, NI, stride=NP), :] for p in range(4)]
        parts.append(jnp.concatenate(rows, axis=0))
    return jnp.concatenate(parts, axis=1)


def pick(index, table):
    out = table[-1]
    for at in range(len(table) - 2, -1, -1):
        out = jnp.where(index == at, table[at], out)
    return jnp.int32(out)


def kernel(
    raw_hbm, c_hbm, m_hbm, occ_ref, virt_hbm, out_ref,
    raw_v, c_v, virt_v, mbuf, hsend, hx, sbuf, fbuf, jhi, jlo, thi, tlo, esend, ebuf, g, grecv, tbuf,
    local_sem, a2a_send, a2a_recv, m_send, m_recv, e_send, e_recv, x_send, x_recv,
    s_send, s_recv, f_send, f_recv, p_send, d_send, d_recv, g_send, g_recv,
):
    z, yh, co = lax.axis_index("z"), lax.axis_index("yh"), lax.axis_index("co")
    yl, x = lax.axis_index("yl"), lax.axis_index("x")
    me = (z * YH + yh) * CO + co
    chip = z * YH + yh
    rep = yl * X + x
    is_root = rep == HOLDER[0]

    def remote(src, dst, ss, rs, **where):
        return pltpu.make_async_remote_copy(
            src_ref=src, dst_ref=dst, send_sem=ss, recv_sem=rs, device_id=where, device_id_type=MESH
        )

    c_copy = pltpu.make_async_copy(c_hbm, c_v, local_sem.at[5])
    c_copy.start()
    raw_copies = []
    for part in range(4):
        raw_copies.append(
            pltpu.make_async_copy(raw_hbm.at[:, pl.ds(128 * part, 128)], raw_v.at[part], local_sem.at[1 + part])
        )
        raw_copies[-1].start()
    m_copy = pltpu.make_async_copy(m_hbm, mbuf.at[yl], local_sem.at[0])
    m_copy.start()
    virt_copy = pltpu.make_async_copy(virt_hbm, virt_v, local_sem.at[6])
    virt_copy.start()

    zs = [lax.rem(z + step, Z) for step in range(Z)]
    yhs = [lax.rem(yh + step, YH) for step in range(YH)]
    cos = [co, 1 - co]
    yls = [yl, 1 - yl]
    xs = [lax.rem(x + step, X) for step in range(X)]
    across_blk = [(a, b, c) for a in (4, 3, 5, 2, 6, 1, 7, 0) for b in (2, 1, 3, 0) for c in (0, 1)][:-2] + [(0, 0, 1)]
    across_plane = [(a, b, c) for a in (2, 1, 3, 0) for b in (0, 1) for c in (2, 1, 3, 0) if (b, c) != (0, 0)]

    barrier = pltpu.get_barrier_semaphore()
    for a, b, c in across_blk:
        pl.semaphore_signal(
            barrier, inc=1, device_id={"z": zs[a], "yh": yhs[b], "co": cos[c]}, device_id_type=MESH
        )
    for a, b, c in across_plane:
        pl.semaphore_signal(
            barrier, inc=1, device_id={"yh": yhs[a], "yl": yls[b], "x": xs[c]}, device_id_type=MESH
        )

    esend[...] = jnp.full((8, 128), occ_ref[0], F32)

    c_copy.wait()
    c_high, c_low = halves(c_v[...].T)
    for copy in raw_copies:
        copy.wait()
    total = jnp.zeros((4 * NI, 128), F32)
    for k in range(4):
        place = (
            lax.broadcasted_iota(jnp.int32, (NA, 128), 1) == lax.broadcasted_iota(jnp.int32, (NA, 128), 0) + NA * k
        ).astype(F32).astype(BF16)
        right = (mm(c_high, place).astype(BF16), mm(c_low, place).astype(BF16))
        rows = strided(raw_v, 4, k)
        total = total + mm3(halves(rows), right)
    for p in range(4):
        hsend[:, p, :] = total[NI * p : NI * (p + 1)]

    pl.semaphore_wait(barrier, len(across_blk) + len(across_plane))

    for a, b, c in across_blk:
        other = (zs[a] * YH + yhs[b]) * CO + cos[c]
        remote(hsend.at[other], hx.at[x, me], a2a_send, a2a_recv, z=zs[a], yh=yhs[b], co=cos[c]).start()
    hx[x, me] = hsend[me]

    y = yh * YL + yl
    metric = []
    for side, to in ((0, lax.rem(y + 1, 8)), (1, lax.rem(y + 7, 8))):
        rows_of = pl.ds(side * 512, 512)
        copy = remote(
            m_hbm.at[rows_of], mbuf.at[yl, rows_of], m_send.at[side], m_recv.at[side],
            yh=to // YL, yl=lax.rem(to, YL),
        )
        copy.start()
        metric.append(copy)

    distance = pick(rep, DISTANCE)
    ahead = chip + distance
    energies = []
    for core in range(CO):
        energies.append((
            jnp.logical_not(is_root),
            remote(
                esend, ebuf.at[co], e_send.at[core], e_recv.at[co],
                z=lax.rem(ahead // YH, Z), yh=lax.rem(ahead, YH), co=jnp.int32(core),
            ),
        ))
    energies.append((
        jnp.logical_and(is_root, co == 1),
        remote(esend, ebuf.at[1], e_send.at[0], e_recv.at[1], z=lax.rem(z + 2, Z), co=jnp.int32(0)),
    ))
    energies.append((
        jnp.logical_and(is_root, co == 0),
        remote(esend, ebuf.at[0], e_send.at[0], e_recv.at[0], co=jnp.int32(1)),
    ))
    for when, copy in energies:
        @pl.when(when)
        def _(copy=copy):
            copy.start()

    @pl.when(is_root)
    def _():
        ebuf[co] = esend[...]

    remote(
        hx.at[x, pl.ds(0, NI - 1)], hx.at[x, pl.ds(0, NI - 1)], a2a_send, a2a_recv, co=1 - co
    ).wait_recv()
    gathers = []
    for step in (2, 1, 3):
        copy = remote(hx.at[x], hx.at[x], x_send.at[step], x_recv.at[x], x=lax.rem(x + step, X))
        copy.start()
        gathers.append(copy)
    m_copy.wait()
    for copy in metric:
        copy.wait_recv()
    for step in (1, 3, 2):
        origin = lax.rem(x + step, X)
        remote(hx.at[origin], hx.at[origin], x_send.at[step], x_recv.at[origin], x=origin).wait_recv()

    turned = []
    for xx in range(X):
        block = jnp.concatenate([hx[xx, :, p, :] for p in range(4)], axis=0)
        turned.append(block.T)
    part = jnp.zeros((128, 256), F32)
    for k in range(4):
        left = jnp.concatenate([t[NA * k : NA * (k + 1), :] for t in turned], axis=0)
        right = strided(mbuf, 2, k)
        part = part + mm3(halves(left), halves(right))
    my_rows = pl.ds(pl.multiple_of(yl * 128, 128), 128)
    sbuf[0] = part
    fbuf[0, x, my_rows, :] = part

    up = lax.rem(z + 1, Z)
    sends = []

    def launch(copy, when=None):
        sends.append((copy, when))
        if when is None:
            copy.start()
        else:
            @pl.when(when)
            def _():
                copy.start()

    def to_holder(slot, index, steps, holder, when=None):
        launch(
            remote(
                sbuf.at[slot], fbuf.at[1 + co, x, my_rows], p_send.at[index], f_recv.at[1, rep],
                yh=lax.rem(yh + steps, YH), yl=holder // X, x=lax.rem(holder, X),
            ),
            when,
        )

    launch(remote(sbuf.at[0], sbuf.at[1], s_send.at[0], s_recv.at[0], z=up))
    launch(remote(sbuf.at[0], sbuf.at[2], s_send.at[1], s_recv.at[1], z=zs[2]))
    for step in range(1, 4):
        to_holder(0, step - 1, step, jnp.int32(HOLDER[step]), yh + step < YH)
    other_rows = pl.ds(pl.multiple_of((1 - yl) * 128, 128), 128)
    twin = (1 - yl) * X + x
    launch(
        remote(
            fbuf.at[0, x, my_rows], fbuf.at[0, x, my_rows], f_send.at[0], f_recv.at[0, rep], yl=1 - yl
        )
    )
    remote(sbuf.at[1], sbuf.at[1], s_send.at[0], s_recv.at[0], z=up).wait_recv()
    for step in (2, 1, 3):
        holder = jnp.where(yh + step >= YH, HOLDER[step], HOLDER[step + 4])
        to_holder(1, 3 + step, step, holder)
    to_holder(1, 3, 0, jnp.int32(HOLDER[4]), rep != HOLDER[4])

    @pl.when(rep == HOLDER[4])
    def _():
        fbuf[1 + co, x, my_rows, :] = sbuf[1]

    for step in (2, 1, 3):
        launch(
            remote(
                fbuf.at[0, x, my_rows], fbuf.at[0, x, my_rows], f_send.at[step], f_recv.at[0, rep], x=xs[step]
            )
        )
    remote(
        fbuf.at[0, x, other_rows], fbuf.at[0, x, other_rows], f_send.at[0], f_recv.at[0, twin], co=1 - co
    ).wait_recv()
    for step in (2, 1, 3):
        launch(
            remote(
                fbuf.at[0, x, other_rows], fbuf.at[0, x, other_rows], f_send.at[4 + step], f_recv.at[0, twin],
                x=xs[step],
            )
        )

    remote(sbuf.at[2], sbuf.at[2], s_send.at[1], s_recv.at[1], z=up).wait_recv()
    for step in (2, 1, 3):
        to_holder(2, 7 + step, step, jnp.int32(HOLDER[step + 4]), yh + step >= YH)
    to_holder(2, 7, 0, jnp.int32(HOLDER[0]), jnp.logical_and(co == 1, jnp.logical_not(is_root)))

    @pl.when(jnp.logical_and(is_root, co == 1))
    def _():
        fbuf[2, x, my_rows, :] = sbuf[2]

    own_first = jnp.logical_and(is_root, co == 0)
    kind = jnp.where(own_first, 0, 1)
    source = jnp.where(own_first, 0, 1 + co)
    here = jnp.logical_or(is_root, rep == HOLDER[4])

    def block_of(slot, origin):
        return fbuf.at[slot, lax.rem(origin, X), pl.ds(pl.multiple_of(origin // X * 128, 128), 128)]

    def pass_on(t, _):
        origin = lax.rem(rep + t, 8)

        known = jnp.logical_or(jnp.logical_and(origin == rep, here), jnp.logical_and(origin == twin, own_first))

        @pl.when(jnp.logical_not(known))
        def _():
            remote(
                block_of(source, origin), block_of(source, origin), f_send.at[0], f_recv.at[kind, origin],
                co=1 - co,
            ).wait_recv()

        remote(
            block_of(source, origin), block_of(1 + co, origin), d_send.at[origin], d_recv.at[origin], co=1 - co
        ).start()
        return 0

    lax.fori_loop(0, 8, pass_on, 0)

    def own_arrived(t, _):
        origin = lax.rem(rep + t, 8)

        @pl.when(origin != twin)
        def _():
            remote(
                block_of(0, origin), block_of(0, origin), f_send.at[0], f_recv.at[0, origin], co=1 - co
            ).wait_recv()

        return 0

    @pl.when(jnp.logical_not(own_first))
    def _():
        lax.fori_loop(1, 8, own_arrived, 0)

    for core in range(CO):
        expected = jnp.logical_or(jnp.logical_not(is_root), co != core)

        @pl.when(expected)
        def _(core=core):
            remote(esend, ebuf.at[core], e_send.at[0], e_recv.at[core], co=1 - co).wait_recv()

    virt_copy.wait()
    row = jnp.broadcast_to(virt_v[...], (256, 256))
    spread = row + row.T - occ_ref[0]

    def pair(order):
        which = co if order == 0 else 1 - co
        slot = jnp.where(jnp.logical_and(is_root, co == which), 0, 1 + which)
        coulomb = jnp.zeros((256, 256), F32)
        for xx in range(X):
            ih, il = halves(fbuf[0, xx])
            jh, jl = halves(fbuf[slot, xx])
            jhi[order, xx] = jh
            jlo[order, xx] = jl
            coulomb = coulomb + (mm_nt(ih, jh) + (mm_nt(ih, jl) + mm_nt(il, jh)))
        amplitude = (2.0 * coulomb - coulomb.T) / (spread - ebuf[which][0:1, 0:1])
        th, tl = halves(amplitude)
        thi[order] = th
        tlo[order] = tl

    pair(0)

    def twin_arrived(t, _):
        remote(
            block_of(2 - co, t), block_of(2 - co, t), d_send.at[t], d_recv.at[t], co=1 - co
        ).wait_recv()
        return 0

    lax.fori_loop(0, 8, twin_arrived, 0)
    pair(1)

    def to_column(step, half, index):
        launch(
            remote(
                g.at[xs[step], half], grecv.at[x, half], g_send.at[step, index], g_recv.at[x, index], x=xs[step]
            )
        )

    for step in (2, 1, 3, 0):
        xx = xs[step]
        block = jnp.zeros((256, 256), F32)
        for order in range(2):
            block = block + mm3((thi[order], tlo[order]), (jhi[order, xx], jlo[order, xx]))
        for half in range(YL):
            g[xx, half] = block[:, half * NQ : (half + 1) * NQ]
        if step:
            to_column(step, 1 - yl, 0)
    for step in (2, 1, 3):
        to_column(step, yl, 1)

    def column_sum(half, index):
        for step in (1, 3, 2):
            block = grecv.at[xs[step], half]
            remote(block, block, g_send.at[0, 0], g_recv.at[xs[step], index], co=1 - co).wait_recv()
        result = g[x, half]
        for step in (1, 2, 3):
            result = result + grecv[xs[step], half]
        return result

    tbuf[0] = column_sum(1 - yl, 0)
    launch(remote(tbuf.at[0], tbuf.at[1], g_send.at[0, 0], g_recv.at[x, 0], yl=1 - yl))
    result = column_sum(yl, 1)
    remote(tbuf.at[1], tbuf.at[1], g_send.at[0, 0], g_recv.at[x, 0], co=1 - co).wait_recv()
    out_ref[...] = result + tbuf[1]

    remote(
        hsend.at[pl.ds(0, NI - 1)], hx.at[x, pl.ds(0, NI - 1)], a2a_send, a2a_recv, co=1 - co
    ).wait_send()
    for copy in metric + gathers:
        copy.wait_send()
    for when, copy in energies:
        @pl.when(when)
        def _(copy=copy):
            copy.wait_send()
    for copy, when in sends:
        if when is None:
            copy.wait_send()
        else:
            @pl.when(when)
            def _(copy=copy):
                copy.wait_send()

    def passed(t, _):
        remote(
            block_of(source, t), block_of(1 + co, t), d_send.at[t], d_recv.at[t], co=1 - co
        ).wait_send()
        return 0

    lax.fori_loop(0, 8, passed, 0)


def per_device(raw_integrals, virtual_coeffs, metric_root, occ_energies, virt_energies):
    vmem = pl.BlockSpec(memory_space=pltpu.VMEM)
    anywhere = pl.BlockSpec(memory_space=pl.ANY)
    dma = pltpu.SemaphoreType.DMA
    out = pl.pallas_call(
        kernel,
        out_shape=jax.ShapeDtypeStruct((256, NQ), F32),
        in_specs=[anywhere, anywhere, anywhere, pl.BlockSpec(memory_space=pltpu.SMEM), anywhere],
        out_specs=vmem,
        scratch_shapes=[
            pltpu.VMEM((4, NI * NP, 128), F32),
            pltpu.VMEM((NA, NM), F32),
            pltpu.VMEM((1, 256), F32),
            pltpu.VMEM((YL, 1024, NQ), F32),
            pltpu.VMEM((NI, 4, 128), F32),
            pltpu.VMEM((X, NI, 4, 128), F32),
            pltpu.VMEM((3, 128, 256), F32),
            pltpu.VMEM((3, X, 256, 256), F32),
            pltpu.VMEM((2, X, 256, 256), BF16),
            pltpu.VMEM((2, X, 256, 256), BF16),
            pltpu.VMEM((2, 256, 256), BF16),
            pltpu.VMEM((2, 256, 256), BF16),
            pltpu.VMEM((8, 128), F32),
            pltpu.VMEM((2, 8, 128), F32),
            pltpu.VMEM((X, YL, 256, NQ), F32),
            pltpu.VMEM((X, YL, 256, NQ), F32),
            pltpu.VMEM((2, 256, NQ), F32),
            dma((7,)), dma, dma, dma((2,)), dma((2,)), dma((2,)), dma((2,)), dma((4,)), dma((4,)),
            dma((2,)), dma((2,)), dma((8,)), dma((2, 8)), dma((11,)), dma((8,)), dma((8,)), dma((X, 2)), dma((X, 2)),
        ],
        compiler_params=pltpu.CompilerParams(
            collective_id=0, has_side_effects=True, vmem_limit_bytes=67043328
        ),
        name="gradient_density",
    )(
        raw_integrals.reshape(NI * NP, NM), virtual_coeffs.T, metric_root,
        occ_energies, virt_energies.reshape(1, 256),
    )
    return out[None]


def solution(mesh):
    finer = Mesh(mesh.devices.reshape(Z, YH, CO, YL, X), BLK + REP)
    return jax.shard_map(
        per_device,
        mesh=finer,
        in_specs=(P(None, BLK, None), P(None, REP), P(None, REP), P(BLK), P()),
        out_specs=P(BLK, None, REP),
        check_vma=False,
    )
```

```python
import jax
import jax.numpy as jnp
from jax import lax
from jax.experimental import pallas as pl
from jax.experimental.pallas import tpu as pltpu
from jax.sharding import Mesh
from jax.sharding import PartitionSpec as P

F32 = jnp.float32
BF16 = jnp.bfloat16
MESH = pl.DeviceIdType.MESH
Z, YH, CO, YL, X = 8, 4, 2, 2, 4
BLK = ("z", "yh", "co")
REP = ("yl", "x")
NI, NP, NM, NA, NQ = 64, 16, 512, 32, 128
HOLDER = (1, 2, 0, 6, 4, 3, 5, 7)
DISTANCE = (2, 0, 1, 5, 4, 6, 3, 7)


def halves(v):
    high = v.astype(BF16)
    return high, (v - high.astype(F32)).astype(BF16)


def mm(a, b):
    return jnp.dot(a, b, preferred_element_type=F32)


def mm3(a, b):
    return mm(a[0], b[0]) + (mm(a[0], b[1]) + mm(a[1], b[0]))


def mm_nt(a, b):
    return lax.dot_general(a, b, (((1,), (1,)), ((), ())), preferred_element_type=F32)


def strided(ref, count, k):
    parts = []
    for part in range(count):
        rows = [ref[part, pl.ds(4 * p + k, NI, stride=NP), :] for p in range(4)]
        parts.append(jnp.concatenate(rows, axis=0))
    return jnp.concatenate(parts, axis=1)


def pick(index, table):
    out = table[-1]
    for at in range(len(table) - 2, -1, -1):
        out = jnp.where(index == at, table[at], out)
    return jnp.int32(out)


def kernel(
    raw_hbm, c_hbm, m_hbm, occ_ref, virt_hbm, out_ref,
    raw_v, c_v, virt_v, mbuf, hsend, hx, sbuf, fbuf, jhi, jlo, thi, tlo, esend, ebuf, g, grecv, tbuf,
    local_sem, a2a_send, a2a_recv, m_send, m_recv, e_send, e_recv, x_send, x_recv,
    s_send, s_recv, f_send, f_recv, p_send, d_send, d_recv, g_send, g_recv,
):
    z, yh, co = lax.axis_index("z"), lax.axis_index("yh"), lax.axis_index("co")
    yl, x = lax.axis_index("yl"), lax.axis_index("x")
    me = (z * YH + yh) * CO + co
    chip = z * YH + yh
    rep = yl * X + x
    is_root = rep == HOLDER[0]

    def remote(src, dst, ss, rs, **where):
        return pltpu.make_async_remote_copy(
            src_ref=src, dst_ref=dst, send_sem=ss, recv_sem=rs, device_id=where, device_id_type=MESH
        )

    c_copy = pltpu.make_async_copy(c_hbm, c_v, local_sem.at[5])
    c_copy.start()
    raw_copies = []
    for part in range(4):
        raw_copies.append(
            pltpu.make_async_copy(raw_hbm.at[:, pl.ds(128 * part, 128)], raw_v.at[part], local_sem.at[1 + part])
        )
        raw_copies[-1].start()
    m_copy = pltpu.make_async_copy(m_hbm, mbuf.at[yl], local_sem.at[0])
    m_copy.start()
    virt_copy = pltpu.make_async_copy(virt_hbm, virt_v, local_sem.at[6])
    virt_copy.start()

    zs = [lax.rem(z + step, Z) for step in range(Z)]
    yhs = [lax.rem(yh + step, YH) for step in range(YH)]
    cos = [co, 1 - co]
    yls = [yl, 1 - yl]
    xs = [lax.rem(x + step, X) for step in range(X)]
    across_blk = [(a, b, c) for a in (4, 3, 5, 2, 6, 1, 7, 0) for b in (2, 1, 3, 0) for c in (0, 1)][:-2] + [(0, 0, 1)]
    across_plane = [(a, b, c) for a in (2, 1, 3, 0) for b in (0, 1) for c in (2, 1, 3, 0) if (b, c) != (0, 0)]

    barrier = pltpu.get_barrier_semaphore()
    for a, b, c in across_blk:
        pl.semaphore_signal(
            barrier, inc=1, device_id={"z": zs[a], "yh": yhs[b], "co": cos[c]}, device_id_type=MESH
        )
    for a, b, c in across_plane:
        pl.semaphore_signal(
            barrier, inc=1, device_id={"yh": yhs[a], "yl": yls[b], "x": xs[c]}, device_id_type=MESH
        )

    esend[...] = jnp.full((8, 128), occ_ref[0], F32)

    c_copy.wait()
    c_high, c_low = halves(c_v[...].T)
    for copy in raw_copies:
        copy.wait()
    total = jnp.zeros((4 * NI, 128), F32)
    for k in range(4):
        place = (
            lax.broadcasted_iota(jnp.int32, (NA, 128), 1) == lax.broadcasted_iota(jnp.int32, (NA, 128), 0) + NA * k
        ).astype(F32).astype(BF16)
        right = (mm(c_high, place).astype(BF16), mm(c_low, place).astype(BF16))
        rows = strided(raw_v, 4, k)
        total = total + mm3(halves(rows), right)
    for p in range(4):
        hsend[:, p, :] = total[NI * p : NI * (p + 1)]

    pl.semaphore_wait(barrier, len(across_blk) + len(across_plane))

    for a, b, c in across_blk:
        other = (zs[a] * YH + yhs[b]) * CO + cos[c]
        remote(hsend.at[other], hx.at[x, me], a2a_send, a2a_recv, z=zs[a], yh=yhs[b], co=cos[c]).start()
    hx[x, me] = hsend[me]

    y = yh * YL + yl
    metric = []
    for side, to in ((0, lax.rem(y + 1, 8)), (1, lax.rem(y + 7, 8))):
        rows_of = pl.ds(side * 512, 512)
        copy = remote(
            m_hbm.at[rows_of], mbuf.at[yl, rows_of], m_send.at[side], m_recv.at[side],
            yh=to // YL, yl=lax.rem(to, YL),
        )
        copy.start()
        metric.append(copy)

    distance = pick(rep, DISTANCE)
    ahead = chip + distance
    energies = []
    for core in range(CO):
        energies.append((
            jnp.logical_not(is_root),
            remote(
                esend, ebuf.at[co], e_send.at[core], e_recv.at[co],
                z=lax.rem(ahead // YH, Z), yh=lax.rem(ahead, YH), co=jnp.int32(core),
            ),
        ))
    energies.append((
        jnp.logical_and(is_root, co == 1),
        remote(esend, ebuf.at[1], e_send.at[0], e_recv.at[1], z=lax.rem(z + 2, Z), co=jnp.int32(0)),
    ))
    energies.append((
        jnp.logical_and(is_root, co == 0),
        remote(esend, ebuf.at[0], e_send.at[0], e_recv.at[0], co=jnp.int32(1)),
    ))
    for when, copy in energies:
        @pl.when(when)
        def _(copy=copy):
            copy.start()

    @pl.when(is_root)
    def _():
        ebuf[co] = esend[...]

    remote(
        hx.at[x, pl.ds(0, NI - 1)], hx.at[x, pl.ds(0, NI - 1)], a2a_send, a2a_recv, co=1 - co
    ).wait_recv()
    gathers = []
    for step in (2, 1, 3):
        copy = remote(hx.at[x], hx.at[x], x_send.at[step], x_recv.at[x], x=lax.rem(x + step, X))
        copy.start()
        gathers.append(copy)
    m_copy.wait()
    for copy in metric:
        copy.wait_recv()
    for step in (1, 3, 2):
        origin = lax.rem(x + step, X)
        remote(hx.at[origin], hx.at[origin], x_send.at[step], x_recv.at[origin], x=origin).wait_recv()

    turned = []
    for xx in range(X):
        block = jnp.concatenate([hx[xx, :, p, :] for p in range(4)], axis=0)
        turned.append(block.T)
    part = jnp.zeros((128, 256), F32)
    for k in range(4):
        left = jnp.concatenate([t[NA * k : NA * (k + 1), :] for t in turned], axis=0)
        right = strided(mbuf, 2, k)
        part = part + mm3(halves(left), halves(right))
    my_rows = pl.ds(pl.multiple_of(yl * 128, 128), 128)
    sbuf[0] = part
    fbuf[0, x, my_rows, :] = part

    up = lax.rem(z + 1, Z)
    sends = []

    def launch(copy, when=None):
        sends.append((copy, when))
        if when is None:
            copy.start()
        else:
            @pl.when(when)
            def _():
                copy.start()

    def to_holder(slot, index, steps, holder, when=None):
        launch(
            remote(
                sbuf.at[slot], fbuf.at[1 + co, x, my_rows], p_send.at[index], f_recv.at[1, rep],
                yh=lax.rem(yh + steps, YH), yl=holder // X, x=lax.rem(holder, X),
            ),
            when,
        )

    launch(remote(sbuf.at[0], sbuf.at[1], s_send.at[0], s_recv.at[0], z=up))
    launch(remote(sbuf.at[0], sbuf.at[2], s_send.at[1], s_recv.at[1], z=zs[2]))
    for step in range(1, 4):
        to_holder(0, step - 1, step, jnp.int32(HOLDER[step]), yh + step < YH)
    other_rows = pl.ds(pl.multiple_of((1 - yl) * 128, 128), 128)
    twin = (1 - yl) * X + x
    launch(
        remote(
            fbuf.at[0, x, my_rows], fbuf.at[0, x, my_rows], f_send.at[0], f_recv.at[0, rep], yl=1 - yl
        )
    )
    remote(sbuf.at[1], sbuf.at[1], s_send.at[0], s_recv.at[0], z=up).wait_recv()
    for step in (2, 1, 3):
        holder = jnp.where(yh + step >= YH, HOLDER[step], HOLDER[step + 4])
        to_holder(1, 3 + step, step, holder)
    to_holder(1, 3, 0, jnp.int32(HOLDER[4]), rep != HOLDER[4])

    @pl.when(rep == HOLDER[4])
    def _():
        fbuf[1 + co, x, my_rows, :] = sbuf[1]

    for step in (2, 1, 3):
        launch(
            remote(
                fbuf.at[0, x, my_rows], fbuf.at[0, x, my_rows], f_send.at[step], f_recv.at[0, rep], x=xs[step]
            )
        )
    remote(
        fbuf.at[0, x, other_rows], fbuf.at[0, x, other_rows], f_send.at[0], f_recv.at[0, twin], co=1 - co
    ).wait_recv()
    for step in (2, 1, 3):
        launch(
            remote(
                fbuf.at[0, x, other_rows], fbuf.at[0, x, other_rows], f_send.at[4 + step], f_recv.at[0, twin],
                x=xs[step],
            )
        )

    remote(sbuf.at[2], sbuf.at[2], s_send.at[1], s_recv.at[1], z=up).wait_recv()
    for step in (2, 1, 3):
        to_holder(2, 7 + step, step, jnp.int32(HOLDER[step + 4]), yh + step >= YH)
    to_holder(2, 7, 0, jnp.int32(HOLDER[0]), jnp.logical_and(co == 1, jnp.logical_not(is_root)))

    @pl.when(jnp.logical_and(is_root, co == 1))
    def _():
        fbuf[2, x, my_rows, :] = sbuf[2]

    own_first = jnp.logical_and(is_root, co == 0)
    kind = jnp.where(own_first, 0, 1)
    source = jnp.where(own_first, 0, 1 + co)
    here = jnp.logical_or(is_root, rep == HOLDER[4])

    def block_of(slot, origin):
        return fbuf.at[slot, lax.rem(origin, X), pl.ds(pl.multiple_of(origin // X * 128, 128), 128)]

    def pass_on(t, _):
        origin = lax.rem(rep + t, 8)

        known = jnp.logical_or(jnp.logical_and(origin == rep, here), jnp.logical_and(origin == twin, own_first))

        @pl.when(jnp.logical_not(known))
        def _():
            remote(
                block_of(source, origin), block_of(source, origin), f_send.at[0], f_recv.at[kind, origin],
                co=1 - co,
            ).wait_recv()

        remote(
            block_of(source, origin), block_of(1 + co, origin), d_send.at[origin], d_recv.at[origin], co=1 - co
        ).start()
        return 0

    lax.fori_loop(0, 8, pass_on, 0)

    def own_arrived(t, _):
        origin = lax.rem(rep + t, 8)

        @pl.when(origin != twin)
        def _():
            remote(
                block_of(0, origin), block_of(0, origin), f_send.at[0], f_recv.at[0, origin], co=1 - co
            ).wait_recv()

        return 0

    @pl.when(jnp.logical_not(own_first))
    def _():
        lax.fori_loop(1, 8, own_arrived, 0)

    for core in range(CO):
        expected = jnp.logical_or(jnp.logical_not(is_root), co != core)

        @pl.when(expected)
        def _(core=core):
            remote(esend, ebuf.at[core], e_send.at[0], e_recv.at[core], co=1 - co).wait_recv()

    virt_copy.wait()
    row = jnp.broadcast_to(virt_v[...], (256, 256))
    spread = row + row.T - occ_ref[0]

    def pair(order):
        which = co if order == 0 else 1 - co
        slot = jnp.where(jnp.logical_and(is_root, co == which), 0, 1 + which)
        coulomb = jnp.zeros((256, 256), F32)
        for xx in range(X):
            ih, il = halves(fbuf[0, xx])
            jh, jl = halves(fbuf[slot, xx])
            jhi[order, xx] = jh
            jlo[order, xx] = jl
            coulomb = coulomb + (mm_nt(ih, jh) + (mm_nt(ih, jl) + mm_nt(il, jh)))
        amplitude = (2.0 * coulomb - coulomb.T) / (spread - ebuf[which][0:1, 0:1])
        th, tl = halves(amplitude)
        thi[order] = th
        tlo[order] = tl

    pair(0)

    def twin_arrived(t, _):
        remote(
            block_of(2 - co, t), block_of(2 - co, t), d_send.at[t], d_recv.at[t], co=1 - co
        ).wait_recv()
        return 0

    lax.fori_loop(0, 8, twin_arrived, 0)
    pair(1)

    def to_column(step, half, index):
        launch(
            remote(
                g.at[xs[step], half], grecv.at[x, half], g_send.at[step, index], g_recv.at[x, index], x=xs[step]
            )
        )

    for step in (2, 1, 3, 0):
        xx = xs[step]
        block = jnp.zeros((256, 256), F32)
        for order in range(2):
            block = block + mm3((thi[order], tlo[order]), (jhi[order, xx], jlo[order, xx]))
        for half in range(YL):
            g[xx, half] = block[:, half * NQ : (half + 1) * NQ]
        if step == 2:
            launch(remote(g.at[xx, 1 - yl], tbuf.at[2], g_send.at[2, 0], g_recv.at[x, 1], yl=1 - yl))
        elif step:
            to_column(step, 1 - yl, 0)
    for step in (1, 3):
        to_column(step, yl, 1)
    remote(tbuf.at[2], tbuf.at[2], g_send.at[0, 0], g_recv.at[x, 1], co=1 - co).wait_recv()
    tbuf[3] = g[xs[2], yl] + tbuf[2]
    launch(remote(tbuf.at[3], grecv.at[x, yl], g_send.at[2, 1], g_recv.at[x, 1], x=xs[2]))

    def column_sum(half, index):
        steps = (1, 3, 2) if index else (1, 3)
        for step in steps:
            block = grecv.at[xs[step], half]
            remote(block, block, g_send.at[0, 0], g_recv.at[xs[step], index], co=1 - co).wait_recv()
        result = g[x, half]
        for step in steps:
            result = result + grecv[xs[step], half]
        return result

    tbuf[0] = column_sum(1 - yl, 0)
    launch(remote(tbuf.at[0], tbuf.at[1], g_send.at[0, 0], g_recv.at[x, 0], yl=1 - yl))
    result = column_sum(yl, 1)
    remote(tbuf.at[1], tbuf.at[1], g_send.at[0, 0], g_recv.at[x, 0], co=1 - co).wait_recv()
    out_ref[...] = result + tbuf[1]

    remote(
        hsend.at[pl.ds(0, NI - 1)], hx.at[x, pl.ds(0, NI - 1)], a2a_send, a2a_recv, co=1 - co
    ).wait_send()
    for copy in metric + gathers:
        copy.wait_send()
    for when, copy in energies:
        @pl.when(when)
        def _(copy=copy):
            copy.wait_send()
    for copy, when in sends:
        if when is None:
            copy.wait_send()
        else:
            @pl.when(when)
            def _(copy=copy):
                copy.wait_send()

    def passed(t, _):
        remote(
            block_of(source, t), block_of(1 + co, t), d_send.at[t], d_recv.at[t], co=1 - co
        ).wait_send()
        return 0

    lax.fori_loop(0, 8, passed, 0)


def per_device(raw_integrals, virtual_coeffs, metric_root, occ_energies, virt_energies):
    vmem = pl.BlockSpec(memory_space=pltpu.VMEM)
    anywhere = pl.BlockSpec(memory_space=pl.ANY)
    dma = pltpu.SemaphoreType.DMA
    out = pl.pallas_call(
        kernel,
        out_shape=jax.ShapeDtypeStruct((256, NQ), F32),
        in_specs=[anywhere, anywhere, anywhere, pl.BlockSpec(memory_space=pltpu.SMEM), anywhere],
        out_specs=vmem,
        scratch_shapes=[
            pltpu.VMEM((4, NI * NP, 128), F32),
            pltpu.VMEM((NA, NM), F32),
            pltpu.VMEM((1, 256), F32),
            pltpu.VMEM((YL, 1024, NQ), F32),
            pltpu.VMEM((NI, 4, 128), F32),
            pltpu.VMEM((X, NI, 4, 128), F32),
            pltpu.VMEM((3, 128, 256), F32),
            pltpu.VMEM((3, X, 256, 256), F32),
            pltpu.VMEM((2, X, 256, 256), BF16),
            pltpu.VMEM((2, X, 256, 256), BF16),
            pltpu.VMEM((2, 256, 256), BF16),
            pltpu.VMEM((2, 256, 256), BF16),
            pltpu.VMEM((8, 128), F32),
            pltpu.VMEM((2, 8, 128), F32),
            pltpu.VMEM((X, YL, 256, NQ), F32),
            pltpu.VMEM((X, YL, 256, NQ), F32),
            pltpu.VMEM((4, 256, NQ), F32),
            dma((7,)), dma, dma, dma((2,)), dma((2,)), dma((2,)), dma((2,)), dma((4,)), dma((4,)),
            dma((2,)), dma((2,)), dma((8,)), dma((2, 8)), dma((11,)), dma((8,)), dma((8,)), dma((X, 2)), dma((X, 2)),
        ],
        compiler_params=pltpu.CompilerParams(
            collective_id=0, has_side_effects=True, vmem_limit_bytes=67043328
        ),
        name="gradient_density",
    )(
        raw_integrals.reshape(NI * NP, NM), virtual_coeffs.T, metric_root,
        occ_energies, virt_energies.reshape(1, 256),
    )
    return out[None]


def solution(mesh):
    finer = Mesh(mesh.devices.reshape(Z, YH, CO, YL, X), BLK + REP)
    return jax.shard_map(
        per_device,
        mesh=finer,
        in_specs=(P(None, BLK, None), P(None, REP), P(None, REP), P(BLK), P()),
        out_specs=P(BLK, None, REP),
        check_vma=False,
    )
```
